8 devices in a mesh: rep: 1 (over z), col: 2 (over y), row: 4 (over x, core).
Axes of the slice: x: 2, y: 2, z: 1, core: 2. Of those that a mesh axis runs over, the one named last changes fastest.
Arguments:
- hidden_0: bfloat16 [16, 6144], P('rep', 'row')
- hidden_1: bfloat16 [16, 6144], P('rep', 'row')
- positions: int32 [16], P(('rep', 'row'))
- lengths: int32 [16], P(('rep', 'row'))
- cache_k: bfloat16 [2, 16, 128, 8, 128], P(None, ('rep', 'row'), None, 'col')
- cache_v: bfloat16 [2, 16, 128, 8, 128], P(None, ('rep', 'row'), None, 'col')
- norm_attn: bfloat16 [2, 6144], P(None, 'row')
- norm_mlp: bfloat16 [2, 6144], P(None, 'row')
- w_query: bfloat16 [2, 6144, 6144], P(None, 'row', 'col')
- w_key: bfloat16 [2, 6144, 1024], P(None, 'row', 'col')
- w_value: bfloat16 [2, 6144, 1024], P(None, 'row', 'col')
- w_out: bfloat16 [2, 6144, 6144], P(None, 'row', 'col')
- w_gate: bfloat16 [2, 6144, 16384], P(None, 'row', 'col')
- w_up: bfloat16 [2, 6144, 16384], P(None, 'row', 'col')
- w_down: bfloat16 [2, 16384, 6144], P(None, 'row', 'col')
Outputs:
- output 1: bfloat16 [16, 6144], P('rep', 'row')
- output 2: bfloat16 [16, 6144], P('rep', 'row')
- output 3: bfloat16 [2, 16, 128, 8, 128], P(None, ('rep', 'row'), None, 'col')
- output 4: bfloat16 [2, 16, 128, 8, 128], P(None, ('rep', 'row'), None, 'col')
All inputs are finite; a program needn't handle non-finite values.
Results may differ from the reference program's by a relative error of at most 0.02.
Values are sent between devices in bfloat16 or wider.
A program may use at most 1 GiB of HBM per device.

```python
import math
import jax
import jax.numpy as jnp
from jax import lax

BATCH = 16
CTX_LEN = 128
D_MODEL = 6144
HEADS = 48
KV_HEADS = 8
HEAD_DIM = 128
FF_DIM = 16384
LAYERS = 2
ROPE_BASE = 1000000
EPS = 1e-05
GROUP_SIZE = HEADS // KV_HEADS
Q_WIDTH = HEADS * HEAD_DIM
KV_WIDTH = KV_HEADS * HEAD_DIM
LEN_BITS = int(math.log2(CTX_LEN))


def draw_lengths(key):
    key_exp, key_len, key_pick, key_pos = jax.random.split(key, 4)
    exponent = jax.random.randint(key_exp, (BATCH,), 0, LEN_BITS + 1)
    length_cap = jnp.minimum(jnp.left_shift(jnp.ones((BATCH,), jnp.int32), exponent), CTX_LEN - 2)
    lengths = 1 + jax.random.randint(key_len, (BATCH,), 0, length_cap)
    shuffled = jax.random.permutation(key_pick, BATCH)
    lengths = lengths.at[shuffled[0]].set(CTX_LEN - 2).at[shuffled[1]].set(1)
    positions = lengths + jax.random.randint(key_pos, (BATCH,), 0, CTX_LEN)
    return positions.astype(jnp.int32), lengths.astype(jnp.int32)


def normal_weight(key, shape, fan_in):
    return (jax.random.normal(key, shape, jnp.float32) * fan_in ** -0.5).astype(jnp.bfloat16)


def setup_inputs(seed: int = 0, part: int = 0) -> dict:
    part_keys = jax.random.split(jax.random.fold_in(jax.random.key(seed), part), 5)
    weight_keys = jax.random.split(jax.random.key(seed + 1), 9)
    positions, lengths = draw_lengths(part_keys[0])
    cache_shape = (LAYERS, BATCH, CTX_LEN, KV_HEADS, HEAD_DIM)
    return {
        'hidden_0': jax.random.normal(part_keys[1], (BATCH, D_MODEL), jnp.float32).astype(jnp.bfloat16),
        'hidden_1': jax.random.normal(part_keys[2], (BATCH, D_MODEL), jnp.float32).astype(jnp.bfloat16),
        'positions': positions,
        'lengths': lengths,
        'cache_k': jax.random.normal(part_keys[3], cache_shape, jnp.float32).astype(jnp.bfloat16),
        'cache_v': jax.random.normal(part_keys[4], cache_shape, jnp.float32).astype(jnp.bfloat16),
        'norm_attn': (1.0 + 0.4 * jax.random.normal(weight_keys[0], (LAYERS, D_MODEL), jnp.float32)).astype(jnp.bfloat16),
        'norm_mlp': (1.0 + 0.4 * jax.random.normal(weight_keys[1], (LAYERS, D_MODEL), jnp.float32)).astype(jnp.bfloat16),
        'w_query': normal_weight(weight_keys[2], (LAYERS, D_MODEL, Q_WIDTH), D_MODEL),
        'w_key': normal_weight(weight_keys[3], (LAYERS, D_MODEL, KV_WIDTH), D_MODEL),
        'w_value': normal_weight(weight_keys[4], (LAYERS, D_MODEL, KV_WIDTH), D_MODEL),
        'w_out': normal_weight(weight_keys[5], (LAYERS, Q_WIDTH, D_MODEL), Q_WIDTH),
        'w_gate': normal_weight(weight_keys[6], (LAYERS, D_MODEL, FF_DIM), D_MODEL),
        'w_up': normal_weight(weight_keys[7], (LAYERS, D_MODEL, FF_DIM), D_MODEL),
        'w_down': normal_weight(weight_keys[8], (LAYERS, FF_DIM, D_MODEL), FF_DIM),
    }


def rms_norm(hidden, gain):
    hidden_f = hidden.astype(jnp.float32)
    scale = lax.rsqrt(jnp.mean(hidden_f * hidden_f, axis=-1, keepdims=True) + EPS)
    return (hidden_f * scale * gain.astype(jnp.float32)).astype(jnp.bfloat16)


def matmul_bf16(left, right):
    return jnp.dot(left, right, preferred_element_type=jnp.float32).astype(jnp.bfloat16)


def rope_rotate(vectors, positions):
    half = HEAD_DIM // 2
    inv_freq = jnp.power(jnp.float32(ROPE_BASE), -jnp.arange(half, dtype=jnp.float32) * 2.0 / HEAD_DIM)
    angles = positions.astype(jnp.float32)[:, None, None] * inv_freq
    cosine = jnp.cos(angles)
    sine = jnp.sin(angles)
    first = vectors[..., :half]
    second = vectors[..., half:]
    return jnp.concatenate([first * cosine - second * sine, second * cosine + first * sine], axis=-1).astype(jnp.bfloat16)


def attend_row(row_inputs):
    query, keys, vals, last_slot = row_inputs
    scores = jnp.einsum('kgd,lkd->kgl', query.astype(jnp.float32), keys.astype(jnp.float32)) * (HEAD_DIM ** -0.5)
    valid = jnp.arange(CTX_LEN)[None, None, :] <= last_slot
    probs = jax.nn.softmax(jnp.where(valid, scores, -jnp.inf), axis=-1).astype(jnp.bfloat16)
    return jnp.einsum('kgl,lkd->kgd', probs.astype(jnp.float32), vals.astype(jnp.float32)).astype(jnp.bfloat16)


def decoder_layer(hidden, layer_weights, keys_layer, vals_layer, positions, slots):
    norm_attn, norm_mlp, w_query, w_key, w_value, w_out, w_gate, w_up, w_down = layer_weights
    batch = hidden.shape[0]
    normed = rms_norm(hidden, norm_attn)
    query = rope_rotate(matmul_bf16(normed, w_query).astype(jnp.float32).reshape(batch, HEADS, HEAD_DIM), positions)
    key_new = rope_rotate(matmul_bf16(normed, w_key).astype(jnp.float32).reshape(batch, KV_HEADS, HEAD_DIM), positions)
    value_new = matmul_bf16(normed, w_value).reshape(batch, KV_HEADS, HEAD_DIM)
    rows = jnp.arange(batch)
    keys_layer = keys_layer.at[rows, slots].set(key_new)
    vals_layer = vals_layer.at[rows, slots].set(value_new)
    attended = lax.map(attend_row, (query.reshape(batch, KV_HEADS, GROUP_SIZE, HEAD_DIM), keys_layer, vals_layer, slots))
    attn_out = matmul_bf16(attended.reshape(batch, Q_WIDTH), w_out)
    hidden = (hidden.astype(jnp.float32) + attn_out.astype(jnp.float32)).astype(jnp.bfloat16)
    normed = rms_norm(hidden, norm_mlp)
    gate = matmul_bf16(normed, w_gate).astype(jnp.float32)
    up_proj = matmul_bf16(normed, w_up).astype(jnp.float32)
    activated = (jax.nn.silu(gate) * up_proj).astype(jnp.bfloat16)
    down_out = matmul_bf16(activated, w_down)
    hidden = (hidden.astype(jnp.float32) + down_out.astype(jnp.float32)).astype(jnp.bfloat16)
    return hidden, keys_layer, vals_layer


def run_step(hidden, positions, slots, cache_k, cache_v, weights):
    def layer_body(carry, layer_inputs):
        layer_weights, keys_layer, vals_layer = layer_inputs
        carry, keys_layer, vals_layer = decoder_layer(carry, layer_weights, keys_layer, vals_layer, positions, slots)
        return carry, (keys_layer, vals_layer)
    hidden, caches = lax.scan(layer_body, hidden, (weights, cache_k, cache_v))
    return hidden, caches[0], caches[1]


def reference(hidden_0, hidden_1, positions, lengths, cache_k, cache_v, norm_attn, norm_mlp, w_query, w_key, w_value, w_out, w_gate, w_up, w_down):
    weights = (norm_attn, norm_mlp, w_query, w_key, w_value, w_out, w_gate, w_up, w_down)
    output_0, cache_k, cache_v = run_step(hidden_0, positions, lengths, cache_k, cache_v, weights)
    output_1, cache_k, cache_v = run_step(hidden_1, positions + 1, lengths + 1, cache_k, cache_v, weights)
    return (output_0, output_1, cache_k, cache_v)
```

```python
import functools

import jax
import jax.numpy as jnp
from jax import lax
from jax.experimental import pallas as pl
from jax.experimental.pallas import tpu as pltpu
from jax.sharding import PartitionSpec as P

ROPE_BASE = 1000000.0
EPS = 1e-05
MESH = pl.DeviceIdType.MESH
F32 = jnp.float32
BF16 = jnp.bfloat16

LAYERS = 2
ROWS = 4
COLS = 2
SEQS = 4
RB = 8
D = 1536
HD = 128
QH = 24
KVH = 4
QW = QH * HD
KVW = KVH * HD
FF = 8192
FK = 4096
WIDTH = 6144
CTX = 128
CW = 512
KD = 1024
NS = 30

QKV_N = QW + 2 * KVW
KINDS = ['k', 'v'] + ['q'] * 6 + ['o'] * 6 + ['g', 'u'] * 16 + ['d'] * 24
INDEX = [0, 0] + list(range(6)) + list(range(6)) + [i // 2 for i in range(32)] + list(range(24))
PER_LAYER = len(KINDS)
TOTAL = LAYERS * PER_LAYER
BASE = {'qkv': 0, 'o': 8, 'gu': 14, 'd': 46}


def chunk_of(seq):
    if seq >= TOTAL:
        return None
    layer, pos = divmod(seq, PER_LAYER)
    return layer, KINDS[pos], INDEX[pos]


def mega_kernel(h0, h1, positions, lengths, ck, cv, na, nm, wq, wk, wv, wo, wg, wu, wd,
                out0, out1, kout, vout,
                wbuf, kbuf, vbuf, hbuf, gabuf, gmbuf, nbuf, abuf, xown,
                q_scr, kn_scr, vn_scr, o_scr, lim_scr, cos_scr, sin_scr,
                is_send, is_recv, xi_send, xi_recv,
                qkv_s, qkv_r, o_s, o_r, gu_s, gu_r, d_s, d_r,
                ao_s, ao_r, x_s, x_r, aa_s, aa_r, st_s, st_r,
                wsem, lsem, csem, isem, xisem, rssem, rrsem, assem, arsem, stsem):
    c = lax.axis_index('col')
    r = lax.axis_index('row')
    rep = lax.axis_index('rep')
    me = c * ROWS + r
    home = c == r // 2

    def dev(cc, rr):
        return (rep, cc, rr)

    small = [pltpu.make_async_copy(h0, hbuf.at[0], lsem.at[0]),
             pltpu.make_async_copy(h1, hbuf.at[1], lsem.at[1]),
             pltpu.make_async_copy(na, gabuf, lsem.at[2]),
             pltpu.make_async_copy(nm, gmbuf, lsem.at[3]),
             pltpu.make_async_copy(ck, kbuf, lsem.at[4]),
             pltpu.make_async_copy(cv, vbuf, lsem.at[5])]
    for copy in small[:4]:
        copy.start()

    def weight_copy(layer, kind, idx, slot):
        if kind == 'd':
            n, k = idx // 4, idx % 4
            src = wd.at[layer, pl.ds(pl.multiple_of(k * KD, KD), KD), pl.ds(pl.multiple_of(n * CW, CW), CW)]
            return pltpu.make_async_copy(src, wbuf.at[slot, pl.ds(0, KD)], wsem.at[slot])
        ref = {'k': wk, 'v': wv, 'q': wq, 'o': wo, 'g': wg, 'u': wu}[kind]
        src = ref.at[layer, :, pl.ds(pl.multiple_of(idx * CW, CW), CW)]
        return pltpu.make_async_copy(src, wbuf.at[slot], wsem.at[slot])

    def weight_wait(down, slot):
        if down:
            pltpu.make_async_copy(wd.at[0, pl.ds(0, KD), pl.ds(0, CW)], wbuf.at[slot, pl.ds(0, KD)], wsem.at[slot]).wait()
        else:
            pltpu.make_async_copy(wq.at[0, :, pl.ds(0, CW)], wbuf.at[slot], wsem.at[slot]).wait()

    def issue_initial(lo, hi):
        seq = lo
        while seq < hi:
            layer, kind, idx = chunk_of(seq)
            weight_copy(layer, kind, idx, seq % NS).start()
            seq += 1

    issue_initial(0, 8)
    for copy in small[4:]:
        copy.start()
    issue_initial(8, NS)

    def run_phase(layer, base, iters, per, down, body):
        start = layer * PER_LAYER + base

        def future(t):
            return [chunk_of(start + t * per + e + NS) for e in range(per)]

        def signature(t):
            return [None if f is None else f[:2] for f in future(t)]

        t = 0
        while t < iters:
            end = t + 1
            while end < iters and signature(end) == signature(t):
                end += 1
            first = future(t)
            step = [0] * per
            if end - t > 1:
                nxt = future(t + 1)
                step = [0 if f is None else g[2] - f[2] for f, g in zip(first, nxt)]
                for tt in range(t, end):
                    for f, s, g in zip(first, step, future(tt)):
                        assert f is None or f[2] + s * (tt - t) == g[2]

            def one(i, carry, t=t, first=first, step=step):
                slots = [lax.rem(start + i * per + e, NS) for e in range(per)]
                for s in slots:
                    weight_wait(down, s)
                body(i, slots)
                for f, st, s in zip(first, step, slots):
                    if f is not None:
                        weight_copy(f[0], f[1], f[2] + st * (i - t), s).start()
                return carry

            if end - t == 1:
                one(t, 0)
            else:
                lax.fori_loop(t, end, one, 0)
            t = end

    def rs_send(send, recv, ssem, rsem, off, value):
        width = value.shape[1]
        cols = pl.ds(pl.multiple_of(off, width), width)
        for p in range(ROWS):
            send[p, :, cols] = value[p * RB:(p + 1) * RB].astype(BF16)
        for d in (2, 3, 1):
            tgt = lax.rem(r + d, ROWS)
            pltpu.make_async_remote_copy(send.at[tgt, :, cols], recv.at[d - 1, :, cols], ssem, rsem,
                                         device_id=dev(c, tgt), device_id_type=MESH).start()

    def rs_wait_recv(recv, ssem, rsem):
        pltpu.make_async_remote_copy(recv, recv, ssem, rsem, device_id=dev(c, r), device_id_type=MESH).wait_recv()

    def rs_wait_send(send, ssem, rsem):
        ref = send.at[pl.ds(0, 3)]
        pltpu.make_async_remote_copy(ref, ref, ssem, rsem, device_id=dev(c, r), device_id_type=MESH).wait_send()

    def rs_sum(send, recv, lo, hi):
        acc = send[r, :, lo:hi].astype(F32)
        for d in range(ROWS - 1):
            acc = acc + recv[d, :, lo:hi].astype(F32)
        return acc

    def a2a_copy(send, recv, ssem, rsem, j, cc):
        return pltpu.make_async_remote_copy(send.at[j], recv.at[r], ssem.at[j * COLS + cc], rsem.at[r],
                                            device_id=dev(cc, 2 * c + j), device_id_type=MESH)

    def a2a_self(j, cc):
        return jnp.logical_and(c == cc, r == 2 * c + j)

    def a2a_send(send, recv, ssem, rsem, j):
        for cc in range(COLS):
            mine = a2a_self(j, cc)

            @pl.when(jnp.logical_not(mine))
            def _():
                a2a_copy(send, recv, ssem, rsem, j, cc).start()

            @pl.when(mine)
            def _():
                recv[r] = send[j]

    def a2a_wait_recv(send, recv, ssem, rsem):
        for s in range(ROWS):
            @pl.when(jnp.logical_not(jnp.logical_and(home, r == s)))
            def _():
                pltpu.make_async_remote_copy(send.at[0], recv.at[s], ssem.at[0], rsem.at[s],
                                             device_id=dev(c, r), device_id_type=MESH).wait_recv()

    def a2a_wait_send(send, recv, ssem, rsem):
        for j in range(2):
            for cc in range(COLS):
                @pl.when(jnp.logical_not(a2a_self(j, cc)))
                def _():
                    a2a_copy(send, recv, ssem, rsem, j, cc).wait_send()

    def stat_copy(send, recv, ssem, rsem, e):
        tgt = lax.rem(me + e, COLS * ROWS)
        return pltpu.make_async_remote_copy(send, recv.at[me], ssem, rsem,
                                            device_id=dev(tgt // ROWS, lax.rem(tgt, ROWS)), device_id_type=MESH)

    barrier = pltpu.get_barrier_semaphore()
    for e in range(1, COLS * ROWS):
        tgt = lax.rem(me + e, COLS * ROWS)
        pl.semaphore_signal(barrier, inc=1, device_id=dev(tgt // ROWS, lax.rem(tgt, ROWS)), device_id_type=MESH)
    pl.semaphore_wait(barrier, COLS * ROWS - 1)

    for copy in small[:4]:
        copy.wait()
    h0v = hbuf[0].astype(F32)
    h1v = hbuf[1].astype(F32)
    blocks = [jnp.concatenate([h0v[4 * p:4 * p + 4], h1v[4 * p:4 * p + 4]], axis=0) for p in range(ROWS)]
    for p in range(ROWS):
        sq = jnp.sum(blocks[p] * blocks[p], axis=1, keepdims=True)
        is_send[p] = jnp.broadcast_to(sq, (RB, 128))
    for d in (2, 3, 1):
        tgt = lax.rem(r + d, ROWS)
        pltpu.make_async_remote_copy(is_send, is_recv.at[d - 1], isem.at[0], isem.at[1],
                                     device_id=dev(c, tgt), device_id_type=MESH).start()
    for p in range(ROWS):
        xi_send[p] = blocks[p].astype(BF16)

    @pl.when(home)
    def _():
        for d in range(1, ROWS):
            tgt = lax.rem(r + d, ROWS)
            pltpu.make_async_remote_copy(xi_send.at[tgt], xi_recv.at[lax.rem(r, 2)], xisem.at[0], xisem.at[1 + lax.rem(r, 2)],
                                         device_id=dev(c, tgt), device_id_type=MESH).start()
        xi_recv[lax.rem(r, 2)] = xi_send[r]

    rowi = lax.broadcasted_iota(jnp.int32, (RB, HD), 0)
    lane = lax.broadcasted_iota(jnp.int32, (RB, HD), 1)
    step_id = (rowi >= SEQS).astype(jnp.int32)
    seq_id = rowi - SEQS * step_id
    pos = step_id
    for b in range(SEQS):
        pos = pos + jnp.where(seq_id == b, positions[b], 0)
    half = (lane >= HD // 2)
    freq_i = jnp.where(half, lane - HD // 2, lane).astype(F32)
    inv_freq = jnp.exp(freq_i * (-13.815510557964274 / 64.0))
    angle = pos.astype(F32) * inv_freq
    cos_scr[...] = jnp.cos(angle)
    sine = jnp.sin(angle)
    sin_scr[...] = jnp.where(half, sine, -sine)

    srow = lax.broadcasted_iota(jnp.int32, (2 * QH, CTX * KVH), 0)
    scol = lax.broadcasted_iota(jnp.int32, (2 * QH, CTX * KVH), 1)
    srow_step = (srow >= QH).astype(jnp.int32)
    srow_h = srow - QH * srow_step
    srow_kv = (srow_h >= 6).astype(jnp.int32) + (srow_h >= 12).astype(jnp.int32) + (srow_h >= 18).astype(jnp.int32)
    slot = jnp.right_shift(scol, 2)
    kv_of = jnp.bitwise_and(scol, 3)
    lim_scr[...] = jnp.where(kv_of == srow_kv, slot - srow_step, 1 << 20)

    pltpu.make_async_remote_copy(is_recv, is_recv, isem.at[0], isem.at[1], device_id=dev(c, r), device_id_type=MESH).wait_recv()

    def normalise(p, xblock, total, gain):
        scale = lax.rsqrt(total * (1.0 / WIDTH) + EPS)[:, :1]
        return xblock * scale * gain

    def put_rows(dst, parts):
        dst[...] = jnp.concatenate(parts, axis=0).astype(BF16)

    gain = gabuf[0:1, :].astype(F32)
    parts = []
    for p in range(ROWS):
        total = is_send[p] + is_recv[0, p] + is_recv[1, p] + is_recv[2, p]
        parts.append(normalise(p, blocks[p], total, gain))
    put_rows(nbuf, parts)

    for copy in small[4:]:
        copy.wait()

    out_copies = []
    for layer in range(LAYERS):
        qs, qr = qkv_s.at[layer], qkv_r.at[layer]
        qsem = (rssem.at[layer, 0], rrsem.at[layer, 0])

        def qkv_body(i, slots):
            lhs = nbuf[...]
            y = [jnp.dot(lhs, wbuf[s], preferred_element_type=F32) for s in slots]
            rs_send(qs, qr, *qsem, i * (2 * CW), jnp.concatenate(y, axis=1))

        run_phase(layer, BASE['qkv'], 4, 2, False, qkv_body)
        rs_wait_recv(qr, *qsem)

        cosv, sinv = cos_scr[...], sin_scr[...]

        def rope(block):
            value = block.astype(BF16).astype(F32)
            return (value * cosv + pltpu.roll(value, HD // 2, 1) * sinv).astype(BF16).astype(F32)

        for h in range(KVH):
            kn_scr[h * RB:(h + 1) * RB, :] = rope(rs_sum(qs, qr, h * HD, (h + 1) * HD))
            vn_scr[h * RB:(h + 1) * RB, :] = rs_sum(qs, qr, KVW + h * HD, KVW + (h + 1) * HD)
        for h in range(QH):
            q_scr[h * RB:(h + 1) * RB, :] = rope(rs_sum(qs, qr, 2 * KVW + h * HD, 2 * KVW + (h + 1) * HD))
        row_slot = jnp.right_shift(lax.broadcasted_iota(jnp.int32, (CTX * KVH, HD), 0), 2)
        for b in range(SEQS):
            length = lengths[b]

            def updated(cache, new_scr):
                value = cache[layer, b].astype(F32)
                for s in range(2):
                    new = new_scr[pl.ds(b + SEQS * s, KVH, stride=RB), :]
                    tile = jnp.concatenate([new, new], axis=0)
                    full = jnp.broadcast_to(tile[None], (CTX * KVH // 8, 8, HD)).reshape(CTX * KVH, HD)
                    value = jnp.where(row_slot == length + s, full, value)
                return value.astype(BF16)

            keys = updated(kbuf, kn_scr)
            vals = updated(vbuf, vn_scr)
            kbuf[layer, b] = keys
            vbuf[layer, b] = vals
            qb = jnp.concatenate([q_scr[pl.ds(b + SEQS * s, QH, stride=RB), :] for s in range(2)], axis=0).astype(BF16)
            scores = lax.dot_general(qb, keys, (((1,), (1,)), ((), ())), preferred_element_type=F32) * (HD ** -0.5)
            scores = jnp.where(lim_scr[...] <= length, scores, -jnp.inf)
            top = jnp.max(scores, axis=1, keepdims=True)
            e = jnp.exp(scores - top)
            probs = (e / jnp.sum(e, axis=1, keepdims=True)).astype(BF16)
            ob = jnp.dot(probs, vals, preferred_element_type=F32)
            for s in range(2):
                o_scr[pl.ds(b + SEQS * s, QH, stride=RB), :] = ob[s * QH:(s + 1) * QH]
        aos, aor = ao_s.at[layer], ao_r.at[layer]
        aosem = (assem.at[layer, 0], arsem.at[layer, 0])
        for j in range(2):
            for h in range(QH // 2):
                hh = j * (QH // 2) + h
                aos[j, :, h * HD:(h + 1) * HD] = o_scr[hh * RB:(hh + 1) * RB, :].astype(BF16)
            a2a_send(aos, aor, *aosem, j)
        for which, (buf, out) in enumerate(((kbuf, kout), (vbuf, vout))):
            copy = pltpu.make_async_copy(buf.at[layer], out.at[layer], csem.at[2 * layer + which])
            copy.start()
            out_copies.append(copy)
        a2a_wait_recv(aos, aor, *aosem)
        put_rows(nbuf, [aor[p].astype(F32) for p in range(ROWS)])

        if layer == 0:
            for j in range(2):
                @pl.when(jnp.logical_not(jnp.logical_and(home, lax.rem(r, 2) == j)))
                def _():
                    pltpu.make_async_remote_copy(xi_send.at[0], xi_recv.at[j], xisem.at[0], xisem.at[1 + j],
                                                 device_id=dev(c, r), device_id_type=MESH).wait_recv()
                xown[:, j * D:(j + 1) * D] = xi_recv[j].astype(F32)

        os_, or_ = o_s.at[layer], o_r.at[layer]
        osem = (rssem.at[layer, 1], rrsem.at[layer, 1])

        def o_body(i, slots):
            lhs = nbuf[...]
            y = [jnp.dot(lhs, wbuf[s], preferred_element_type=F32) for s in slots]
            rs_send(os_, or_, *osem, i * (2 * CW), jnp.concatenate(y, axis=1))

        def residual(send, recv, sems, which):
            rs_wait_recv(recv, *sems)
            xs, xr = x_s.at[layer, which], x_r.at[layer, which]
            xsem = (assem.at[layer, 1 + which], arsem.at[layer, 1 + which])
            squares = jnp.zeros((RB, 128), F32)
            for j in range(2):
                update = rs_sum(send, recv, j * D, (j + 1) * D).astype(BF16).astype(F32)
                x = (xown[:, j * D:(j + 1) * D] + update).astype(BF16)
                xs[j] = x
                x = x.astype(F32)
                xown[:, j * D:(j + 1) * D] = x
                a2a_send(xs, xr, *xsem, j)
                sq = x * x
                for k in range(D // 128):
                    squares = squares + sq[:, k * 128:(k + 1) * 128]
            last = layer == LAYERS - 1 and which == 1
            if not last:
                sts, stv = st_s.at[layer, which], st_r.at[layer, which]
                stat = jnp.broadcast_to(jnp.sum(squares, axis=1, keepdims=True), (RB, 128))
                sts[...] = stat
                stv[me] = stat
                for e in range(1, COLS * ROWS):
                    stat_copy(sts, stv, stsem.at[layer, which, 0], stsem.at[layer, which, 1], e).start()
            a2a_wait_recv(xs, xr, *xsem)
            if last:
                return
            seven = stv.at[pl.ds(0, COLS * ROWS - 1)]
            pltpu.make_async_remote_copy(seven, seven, stsem.at[layer, which, 0], stsem.at[layer, which, 1],
                                         device_id=dev(c, r), device_id_type=MESH).wait_recv()
            g = (gmbuf[layer:layer + 1, :] if which == 0 else gabuf[layer + 1:layer + 2, :]).astype(F32)
            parts = []
            for p in range(ROWS):
                parts.append(normalise(p, xr[p].astype(F32), stv[p] + stv[ROWS + p], g))
            put_rows(nbuf, parts)

        run_phase(layer, BASE['o'], 3, 2, False, o_body)
        residual(os_, or_, osem, 0)

        gs, gr = gu_s.at[layer], gu_r.at[layer]
        gsem = (rssem.at[layer, 2], rrsem.at[layer, 2])

        def gu_body(i, slots):
            lhs = nbuf[...]
            y = [jnp.dot(lhs, wbuf[s], preferred_element_type=F32) for s in slots]
            rs_send(gs, gr, *gsem, i * (2 * CW), jnp.concatenate(y, axis=1))

        run_phase(layer, BASE['gu'], 16, 2, False, gu_body)
        rs_wait_recv(gr, *gsem)
        aas, aar = aa_s.at[layer], aa_r.at[layer]
        aasem = (assem.at[layer, 3], arsem.at[layer, 3])
        for j in range(2):
            for i in range(8):
                lo = (j * 8 + i) * 2 * CW
                gate = rs_sum(gs, gr, lo, lo + CW).astype(BF16).astype(F32)
                up = rs_sum(gs, gr, lo + CW, lo + 2 * CW).astype(BF16).astype(F32)
                aas[j, :, i * CW:(i + 1) * CW] = (gate * jax.nn.sigmoid(gate) * up).astype(BF16)
            a2a_send(aas, aar, *aasem, j)
        a2a_wait_recv(aas, aar, *aasem)
        put_rows(abuf, [aar[p].astype(F32) for p in range(ROWS)])

        ds_, dr_ = d_s.at[layer], d_r.at[layer]
        dsem = (rssem.at[layer, 3], rrsem.at[layer, 3])

        def d_body(i, slots):
            y = jnp.zeros((ROWS * RB, CW), F32)
            for k, s in enumerate(slots):
                y = y + jnp.dot(abuf[:, k * KD:(k + 1) * KD], wbuf[s, 0:KD], preferred_element_type=F32)
            rs_send(ds_, dr_, *dsem, i * CW, y)

        run_phase(layer, BASE['d'], 6, 4, True, d_body)
        residual(ds_, dr_, dsem, 1)

    final = [x_r[LAYERS - 1, 1, p].astype(F32) for p in range(ROWS)]
    out0[...] = jnp.concatenate([f[0:4] for f in final], axis=0).astype(BF16)
    out1[...] = jnp.concatenate([f[4:8] for f in final], axis=0).astype(BF16)

    pltpu.make_async_remote_copy(is_recv, is_recv, isem.at[0], isem.at[1], device_id=dev(c, r), device_id_type=MESH).wait_send()

    @pl.when(home)
    def _():
        three = xi_send.at[pl.ds(0, 3)]
        pltpu.make_async_remote_copy(three, three, xisem.at[0], xisem.at[1], device_id=dev(c, r), device_id_type=MESH).wait_send()

    for layer in range(LAYERS):
        for ph, (send, recv) in enumerate(((qkv_s, qkv_r), (o_s, o_r), (gu_s, gu_r), (d_s, d_r))):
            rs_wait_send(send.at[layer], rssem.at[layer, ph], rrsem.at[layer, ph])
        for ph, (send, recv) in enumerate(((ao_s.at[layer], ao_r.at[layer]), (x_s.at[layer, 0], x_r.at[layer, 0]),
                                           (x_s.at[layer, 1], x_r.at[layer, 1]), (aa_s.at[layer], aa_r.at[layer]))):
            a2a_wait_send(send, recv, assem.at[layer, ph], arsem.at[layer, ph])
        for which in range(2):
            if layer == LAYERS - 1 and which == 1:
                continue
            seven = st_r.at[layer, which, pl.ds(0, COLS * ROWS - 1)]
            pltpu.make_async_remote_copy(seven, seven, stsem.at[layer, which, 0], stsem.at[layer, which, 1],
                                         device_id=dev(c, r), device_id_type=MESH).wait_send()
    for copy in out_copies:
        copy.wait()


def solution(mesh):
    hidden_spec = P('rep', 'row')
    index_spec = P(('rep', 'row'))
    cache_spec = P(None, ('rep', 'row'), None, 'col', None)
    gain_spec = P(None, 'row')
    weight_spec = P(None, 'row', 'col')

    def device_program(hidden_0, hidden_1, positions, lengths, cache_k, cache_v, norm_attn, norm_mlp,
                       w_query, w_key, w_value, w_out, w_gate, w_up, w_down):
        cache_shape = cache_k.shape
        flat = (LAYERS, SEQS, CTX * KVH, HD)
        any_spec = pl.BlockSpec(memory_space=pl.ANY)
        smem = pl.BlockSpec(memory_space=pltpu.SMEM)
        vmem = pl.BlockSpec(memory_space=pltpu.VMEM)
        V = pltpu.VMEM
        DMA = pltpu.SemaphoreType.DMA
        scratch = [
            V((NS, D, CW), BF16), V(flat, BF16), V(flat, BF16), V((2, 16, D), BF16),
            V((LAYERS, D), BF16), V((LAYERS, D), BF16), V((ROWS * RB, D), BF16), V((ROWS * RB, FK), BF16), V((RB, QW), F32),
            V((QH * RB, HD), F32), V((KVH * RB, HD), F32), V((KVH * RB, HD), F32), V((QH * RB, HD), F32),
            V((2 * QH, CTX * KVH), jnp.int32), V((RB, HD), F32), V((RB, HD), F32),
            V((ROWS, RB, 128), F32), V((3, ROWS, RB, 128), F32), V((ROWS, RB, D), BF16), V((2, RB, D), BF16),
            V((LAYERS, ROWS, RB, QKV_N), BF16), V((LAYERS, 3, RB, QKV_N), BF16),
            V((LAYERS, ROWS, RB, QW), BF16), V((LAYERS, 3, RB, QW), BF16),
            V((LAYERS, ROWS, RB, 2 * FF), BF16), V((LAYERS, 3, RB, 2 * FF), BF16),
            V((LAYERS, ROWS, RB, QW), BF16), V((LAYERS, 3, RB, QW), BF16),
            V((LAYERS, 2, RB, D), BF16), V((LAYERS, ROWS, RB, D), BF16),
            V((LAYERS, 2, 2, RB, D), BF16), V((LAYERS, 2, ROWS, RB, D), BF16),
            V((LAYERS, 2, RB, FK), BF16), V((LAYERS, ROWS, RB, FK), BF16),
            V((LAYERS, 2, RB, 128), F32), V((LAYERS, 2, COLS * ROWS, RB, 128), F32),
            DMA((NS,)), DMA((6,)), DMA((4,)), DMA((2,)), DMA((3,)),
            DMA((LAYERS, 4)), DMA((LAYERS, 4)), DMA((LAYERS, 4, 4)), DMA((LAYERS, 4, 4)), DMA((LAYERS, 2, 2)),
        ]
        out = pl.pallas_call(
            mega_kernel,
            out_shape=(jax.ShapeDtypeStruct(hidden_0.shape, BF16), jax.ShapeDtypeStruct(hidden_1.shape, BF16),
                       jax.ShapeDtypeStruct(flat, BF16), jax.ShapeDtypeStruct(flat, BF16)),
            in_specs=[any_spec, any_spec, smem, smem] + [any_spec] * 11,
            out_specs=(vmem, vmem, any_spec, any_spec),
            scratch_shapes=scratch,
            compiler_params=pltpu.CompilerParams(collective_id=0, has_side_effects=True, vmem_limit_bytes=67043328),
        )(hidden_0, hidden_1, positions, lengths, cache_k.reshape(flat), cache_v.reshape(flat), norm_attn, norm_mlp,
          w_query, w_key, w_value, w_out, w_gate, w_up, w_down)
        return out[0], out[1], out[2].reshape(cache_shape), out[3].reshape(cache_shape)

    return jax.shard_map(device_program, mesh=mesh,
                         in_specs=(hidden_spec, hidden_spec, index_spec, index_spec, cache_spec, cache_spec, gain_spec, gain_spec) + (weight_spec,) * 7,
                         out_specs=(hidden_spec, hidden_spec, cache_spec, cache_spec), check_vma=False)
```

```python
import functools

import jax
import jax.numpy as jnp
from jax import lax
from jax.experimental import pallas as pl
from jax.experimental.pallas import tpu as pltpu
from jax.sharding import PartitionSpec as P

ROPE_BASE = 1000000.0
EPS = 1e-05
MESH = pl.DeviceIdType.MESH
F32 = jnp.float32
BF16 = jnp.bfloat16

LAYERS = 2
ROWS = 4
COLS = 2
SEQS = 4
RB = 8
D = 1536
HD = 128
QH = 24
KVH = 4
QW = QH * HD
KVW = KVH * HD
FF = 8192
FK = 4096
WIDTH = 6144
CTX = 128
CW = 512
KD = 1024
NS = 30

QKV_N = QW + 2 * KVW
KINDS = ['k', 'v'] + ['q'] * 6 + ['o'] * 6 + ['g', 'u'] * 16 + ['d'] * 24
INDEX = [0, 0] + list(range(6)) + list(range(6)) + [i // 2 for i in range(32)] + list(range(24))
PER_LAYER = len(KINDS)
TOTAL = LAYERS * PER_LAYER
BASE = {'qkv': 0, 'o': 8, 'gu': 14, 'd': 46}
NP = 4
DN = 6
GT = 8
GB = 4 * CW
LAG = 1
RELAYED = (0, 1, 2)


def chunk_of(seq):
    if seq >= TOTAL:
        return None
    layer, pos = divmod(seq, PER_LAYER)
    return layer, KINDS[pos], INDEX[pos]


def mega_kernel(h0, h1, positions, lengths, ck, cv, na, nm, wq, wk, wv, wo, wg, wu, wd,
                out0, out1, kbuf, vbuf,
                wbuf, hbuf, gabuf, gmbuf, nbuf, abuf, xown,
                q_scr, kn_scr, vn_scr, o_scr, lim_scr, cos_scr, sin_scr,
                is_send, is_recv, xi_send, xi_recv,
                qkv_s, qkv_r, o_s, o_r, gd_s, gd_r, gk, gx_s, gx_r, d_s, d_r, dacc,
                ao_s, ao_r, x_s, x_r, aa_s, aa_r, aa_m, st_s, st_r,
                wsem, lsem, isem, xisem, rssem, rrsem, assem, arsem, stsem, gdsem, gdrem, gxsem, gxrem, acsem, acrem):
    c = lax.axis_index('col')
    r = lax.axis_index('row')
    rep = lax.axis_index('rep')
    me = c * ROWS + r
    home = c == r // 2

    def dev(cc, rr):
        return (rep, cc, rr)

    small = [pltpu.make_async_copy(h0, hbuf.at[0], lsem.at[0]),
             pltpu.make_async_copy(h1, hbuf.at[1], lsem.at[1]),
             pltpu.make_async_copy(na, gabuf, lsem.at[2]),
             pltpu.make_async_copy(nm, gmbuf, lsem.at[3]),
             pltpu.make_async_copy(ck, kbuf, lsem.at[4]),
             pltpu.make_async_copy(cv, vbuf, lsem.at[5])]
    for copy in small[:4]:
        copy.start()

    def weight_copy(layer, kind, idx, slot):
        if kind == 'd':
            k, n = idx // DN, idx % DN
            src = wd.at[layer, pl.ds(pl.multiple_of(k * KD, KD), KD), pl.ds(pl.multiple_of(n * CW, CW), CW)]
            return pltpu.make_async_copy(src, wbuf.at[slot, pl.ds(0, KD)], wsem.at[slot])
        ref = {'k': wk, 'v': wv, 'q': wq, 'o': wo, 'g': wg, 'u': wu}[kind]
        if kind in 'gu':
            idx = 8 * ((idx % 4) // 2) + 2 * (idx // 4) + idx % 2
        src = ref.at[layer, :, pl.ds(pl.multiple_of(idx * CW, CW), CW)]
        return pltpu.make_async_copy(src, wbuf.at[slot], wsem.at[slot])

    def weight_wait(down, slot):
        if down:
            pltpu.make_async_copy(wd.at[0, pl.ds(0, KD), pl.ds(0, CW)], wbuf.at[slot, pl.ds(0, KD)], wsem.at[slot]).wait()
        else:
            pltpu.make_async_copy(wq.at[0, :, pl.ds(0, CW)], wbuf.at[slot], wsem.at[slot]).wait()

    def issue_initial(lo, hi):
        seq = lo
        while seq < hi:
            layer, kind, idx = chunk_of(seq)
            weight_copy(layer, kind, idx, seq % NS).start(priority=1)
            seq += 1

    issue_initial(0, 8)
    for copy in small[4:]:
        copy.start()
    issue_initial(8, NS)

    def run_phase(layer, base, lo, iters, per, down, body):
        start = layer * PER_LAYER + base

        def future(t):
            return [chunk_of(start + t * per + e + NS) for e in range(per)]

        def signature(t):
            return [None if f is None else f[:2] for f in future(t)]

        t = lo
        while t < iters:
            end = t + 1
            while end < iters and signature(end) == signature(t):
                end += 1
            first = future(t)
            step = [0] * per
            if end - t > 1:
                nxt = future(t + 1)
                step = [0 if f is None else g[2] - f[2] for f, g in zip(first, nxt)]
                for tt in range(t, end):
                    for f, s, g in zip(first, step, future(tt)):
                        assert f is None or f[2] + s * (tt - t) == g[2]

            def one(i, carry, t=t, first=first, step=step):
                slots = [lax.rem(start + i * per + e, NS) for e in range(per)]
                for s in slots:
                    weight_wait(down, s)
                body(i, slots)
                for f, st, s in zip(first, step, slots):
                    if f is not None:
                        weight_copy(f[0], f[1], f[2] + st * (i - t), s).start(priority=1)
                return carry

            if end - t == 1:
                one(t, 0)
            else:
                lax.fori_loop(t, end, one, 0)
            t = end

    def rs_send(send, recv, ssem, rsem, off, value):
        width = value.shape[1]
        cols = pl.ds(off if isinstance(off, int) else pl.multiple_of(off, width), width)
        for p in range(ROWS):
            send[p, :, cols] = value[p * RB:(p + 1) * RB].astype(BF16)
        for d in (2, 3, 1):
            tgt = lax.rem(r + d, ROWS)
            pltpu.make_async_remote_copy(send.at[tgt, :, cols], recv.at[d - 1, :, cols], ssem, rsem,
                                         device_id=dev(c, tgt), device_id_type=MESH).start()

    def rs_wait_recv(recv, ssem, rsem):
        pltpu.make_async_remote_copy(recv, recv, ssem, rsem, device_id=dev(c, r), device_id_type=MESH).wait_recv()

    def rs_wait_send(send, ssem, rsem):
        ref = send.at[pl.ds(0, 3)]
        pltpu.make_async_remote_copy(ref, ref, ssem, rsem, device_id=dev(c, r), device_id_type=MESH).wait_send()

    def rs_sum(send, recv, lo, hi):
        acc = send[r, :, lo:hi].astype(F32)
        for d in range(ROWS - 1):
            acc = acc + recv[d, :, lo:hi].astype(F32)
        return acc

    def a2a_copy(send, recv, ssem, rsem, j, cc):
        return pltpu.make_async_remote_copy(send.at[j], recv.at[r], ssem.at[j * COLS + cc], rsem.at[r],
                                            device_id=dev(cc, 2 * c + j), device_id_type=MESH)

    def a2a_self(j, cc):
        return jnp.logical_and(c == cc, r == 2 * c + j)

    def a2a_send(send, recv, ssem, rsem, j):
        for cc in range(COLS):
            mine = a2a_self(j, cc)

            @pl.when(jnp.logical_not(mine))
            def _():
                a2a_copy(send, recv, ssem, rsem, j, cc).start()

            @pl.when(mine)
            def _():
                recv[r] = send[j]

    def a2a_wait_recv(send, recv, ssem, rsem):
        for s in range(ROWS):
            @pl.when(jnp.logical_not(jnp.logical_and(home, r == s)))
            def _():
                pltpu.make_async_remote_copy(send.at[0], recv.at[s], ssem.at[0], rsem.at[s],
                                             device_id=dev(c, r), device_id_type=MESH).wait_recv()

    def a2a_wait_send(send, recv, ssem, rsem):
        for j in range(2):
            for cc in range(COLS):
                @pl.when(jnp.logical_not(a2a_self(j, cc)))
                def _():
                    a2a_copy(send, recv, ssem, rsem, j, cc).wait_send()

    core, chip = lax.rem(r, 2), r // 2
    sibling = r + 1 - 2 * core
    across = 2 * (1 - chip) + core

    def act_near(layer, h, j):
        return pltpu.make_async_remote_copy(aa_s.at[layer, h, j], aa_r.at[layer, h, r], acsem.at[layer, h, j], acrem.at[layer, h, r],
                                            device_id=dev(c, 2 * c + j), device_id_type=MESH)

    def act_far(layer, h, j):
        return pltpu.make_async_remote_copy(aa_s.at[layer, h, j], aa_r.at[layer, h, r], acsem.at[layer, h, 2 + j], acrem.at[layer, h, r],
                                            device_id=dev(1 - c, 2 * c + j), device_id_type=MESH)

    def act_hand(layer, h):
        return pltpu.make_async_remote_copy(aa_s.at[layer, h], aa_m.at[layer, h], acsem.at[layer, h, 4], acrem.at[layer, h, 4],
                                            device_id=dev(1 - c, r), device_id_type=MESH)

    def act_forward(layer, h, j):
        return pltpu.make_async_remote_copy(aa_m.at[layer, h, j], aa_r.at[layer, h, r], acsem.at[layer, h, 5 + j], acrem.at[layer, h, r],
                                            device_id=dev(c, 2 * (1 - c) + j), device_id_type=MESH)

    def act_diag(layer, h, j):
        return pltpu.make_async_remote_copy(aa_s.at[layer, h, j], aa_r.at[layer, h, r], acsem.at[layer, h, 2 + j], acrem.at[layer, h, r],
                                            device_id=dev(1 - c, 2 * c + j), device_id_type=MESH)

    def act_send(layer, h):
        @pl.when(jnp.logical_not(home))
        def _():
            if h in RELAYED:
                act_hand(layer, h).start()
            else:
                for j in range(2):
                    act_diag(layer, h, j).start()
            for j in range(2):
                act_near(layer, h, j).start()

        @pl.when(home)
        def _():
            for j in range(2):
                act_far(layer, h, j).start()
            for j in range(2):
                @pl.when(core != j)
                def _():
                    act_near(layer, h, j).start()

                @pl.when(core == j)
                def _():
                    aa_r[layer, h, r] = aa_s[layer, h, j]

    def act_relay(layer, h):
        if h not in RELAYED:
            return

        @pl.when(home)
        def _():
            act_hand(layer, h).wait_recv()
            for j in range(2):
                act_forward(layer, h, j).start()

    def act_wait(layer, h):
        for s in range(ROWS):
            @pl.when(jnp.logical_not(jnp.logical_and(home, r == s)))
            def _():
                pltpu.make_async_remote_copy(aa_s.at[layer, h, 0], aa_r.at[layer, h, s], acsem.at[layer, h, 0], acrem.at[layer, h, s],
                                             device_id=dev(c, r), device_id_type=MESH).wait_recv()

    def act_wait_send(layer, h):
        @pl.when(jnp.logical_not(home))
        def _():
            if h in RELAYED:
                act_hand(layer, h).wait_send()
            else:
                for j in range(2):
                    act_diag(layer, h, j).wait_send()
            for j in range(2):
                act_near(layer, h, j).wait_send()

        @pl.when(home)
        def _():
            for j in range(2):
                act_far(layer, h, j).wait_send()
                if h in RELAYED:
                    act_forward(layer, h, j).wait_send()

                @pl.when(core != j)
                def _():
                    act_near(layer, h, j).wait_send()

    def stat_copy(send, recv, ssem, rsem, e):
        tgt = lax.rem(me + e, COLS * ROWS)
        return pltpu.make_async_remote_copy(send, recv.at[me], ssem, rsem,
                                            device_id=dev(tgt // ROWS, lax.rem(tgt, ROWS)), device_id_type=MESH)

    barrier = pltpu.get_barrier_semaphore()
    for e in range(1, COLS * ROWS):
        tgt = lax.rem(me + e, COLS * ROWS)
        pl.semaphore_signal(barrier, inc=1, device_id=dev(tgt // ROWS, lax.rem(tgt, ROWS)), device_id_type=MESH)
    pl.semaphore_wait(barrier, COLS * ROWS - 1)

    for copy in small[:4]:
        copy.wait()
    h0v = hbuf[0].astype(F32)
    h1v = hbuf[1].astype(F32)
    blocks = [jnp.concatenate([h0v[4 * p:4 * p + 4], h1v[4 * p:4 * p + 4]], axis=0) for p in range(ROWS)]
    for p in range(ROWS):
        sq = jnp.sum(blocks[p] * blocks[p], axis=1, keepdims=True)
        is_send[p] = jnp.broadcast_to(sq, (RB, 128))
    for d in (2, 3, 1):
        tgt = lax.rem(r + d, ROWS)
        pltpu.make_async_remote_copy(is_send, is_recv.at[d - 1], isem.at[0], isem.at[1],
                                     device_id=dev(c, tgt), device_id_type=MESH).start()
    for p in range(ROWS):
        xi_send[p] = blocks[p].astype(BF16)

    @pl.when(home)
    def _():
        for d in range(1, ROWS):
            tgt = lax.rem(r + d, ROWS)
            pltpu.make_async_remote_copy(xi_send.at[tgt], xi_recv.at[lax.rem(r, 2)], xisem.at[0], xisem.at[1 + lax.rem(r, 2)],
                                         device_id=dev(c, tgt), device_id_type=MESH).start()
        xi_recv[lax.rem(r, 2)] = xi_send[r]

    rowi = lax.broadcasted_iota(jnp.int32, (RB, HD), 0)
    lane = lax.broadcasted_iota(jnp.int32, (RB, HD), 1)
    step_id = (rowi >= SEQS).astype(jnp.int32)
    seq_id = rowi - SEQS * step_id
    pos = step_id
    for b in range(SEQS):
        pos = pos + jnp.where(seq_id == b, positions[b], 0)
    half = (lane >= HD // 2)
    freq_i = jnp.where(half, lane - HD // 2, lane).astype(F32)
    inv_freq = jnp.exp(freq_i * (-13.815510557964274 / 64.0))
    angle = pos.astype(F32) * inv_freq
    cos_scr[...] = jnp.cos(angle)
    sine = jnp.sin(angle)
    sin_scr[...] = jnp.where(half, sine, -sine)

    srow = lax.broadcasted_iota(jnp.int32, (2 * QH, CTX * KVH), 0)
    scol = lax.broadcasted_iota(jnp.int32, (2 * QH, CTX * KVH), 1)
    srow_step = (srow >= QH).astype(jnp.int32)
    srow_h = srow - QH * srow_step
    srow_kv = (srow_h >= 6).astype(jnp.int32) + (srow_h >= 12).astype(jnp.int32) + (srow_h >= 18).astype(jnp.int32)
    slot = jnp.right_shift(scol, 2)
    kv_of = jnp.bitwise_and(scol, 3)
    lim_scr[...] = jnp.where(kv_of == srow_kv, slot - srow_step, 1 << 20)

    pltpu.make_async_remote_copy(is_recv, is_recv, isem.at[0], isem.at[1], device_id=dev(c, r), device_id_type=MESH).wait_recv()

    def normalise(p, xblock, total, gain):
        scale = lax.rsqrt(total * (1.0 / WIDTH) + EPS)[:, :1]
        return xblock * scale * gain

    def put_rows(dst, parts):
        dst[...] = jnp.concatenate(parts, axis=0).astype(BF16)

    gain = gabuf[0:1, :].astype(F32)
    parts = []
    for p in range(ROWS):
        total = is_send[p] + is_recv[0, p] + is_recv[1, p] + is_recv[2, p]
        parts.append(normalise(p, blocks[p], total, gain))
    put_rows(nbuf, parts)

    for copy in small[4:]:
        copy.wait()

    for layer in range(LAYERS):
        qs, qr = qkv_s.at[layer], qkv_r.at[layer]
        qsem = (rssem.at[layer, 0], rrsem.at[layer, 0])

        def qkv_body(i, slots):
            lhs = nbuf[...]
            y = [jnp.dot(lhs, wbuf[s], preferred_element_type=F32) for s in slots]
            rs_send(qs, qr, *qsem, i * (4 * CW), jnp.concatenate(y, axis=1))

        run_phase(layer, BASE['qkv'], 0, 2, 4, False, qkv_body)
        rs_wait_recv(qr, *qsem)

        cosv, sinv = cos_scr[...], sin_scr[...]

        def rope(block):
            value = block.astype(BF16).astype(F32)
            return (value * cosv + pltpu.roll(value, HD // 2, 1) * sinv).astype(BF16).astype(F32)

        for h in range(KVH):
            kn_scr[h * RB:(h + 1) * RB, :] = rope(rs_sum(qs, qr, h * HD, (h + 1) * HD))
            vn_scr[h * RB:(h + 1) * RB, :] = rs_sum(qs, qr, KVW + h * HD, KVW + (h + 1) * HD)
        for h in range(QH):
            q_scr[h * RB:(h + 1) * RB, :] = rope(rs_sum(qs, qr, 2 * KVW + h * HD, 2 * KVW + (h + 1) * HD))
        row_slot = jnp.right_shift(lax.broadcasted_iota(jnp.int32, (CTX * KVH, HD), 0), 2)
        for b in range(SEQS):
            length = lengths[b]

            def updated(cache, new_scr):
                value = cache[layer, b].astype(F32)
                for s in range(2):
                    new = new_scr[pl.ds(b + SEQS * s, KVH, stride=RB), :]
                    tile = jnp.concatenate([new, new], axis=0)
                    full = jnp.broadcast_to(tile[None], (CTX * KVH // 8, 8, HD)).reshape(CTX * KVH, HD)
                    value = jnp.where(row_slot == length + s, full, value)
                return value.astype(BF16)

            keys = updated(kbuf, kn_scr)
            vals = updated(vbuf, vn_scr)
            kbuf[layer, b] = keys
            vbuf[layer, b] = vals
            qb = jnp.concatenate([q_scr[pl.ds(b + SEQS * s, QH, stride=RB), :] for s in range(2)], axis=0).astype(BF16)
            scores = lax.dot_general(qb, keys, (((1,), (1,)), ((), ())), preferred_element_type=F32) * (HD ** -0.5)
            scores = jnp.where(lim_scr[...] <= length, scores, -jnp.inf)
            top = jnp.max(scores, axis=1, keepdims=True)
            e = jnp.exp(scores - top)
            probs = (e / jnp.sum(e, axis=1, keepdims=True)).astype(BF16)
            ob = jnp.dot(probs, vals, preferred_element_type=F32)
            for s in range(2):
                o_scr[pl.ds(b + SEQS * s, QH, stride=RB), :] = ob[s * QH:(s + 1) * QH]
        aos, aor = ao_s.at[layer], ao_r.at[layer]
        aosem = (assem.at[layer, 0], arsem.at[layer, 0])
        for j in range(2):
            for h in range(QH // 2):
                hh = j * (QH // 2) + h
                aos[j, :, h * HD:(h + 1) * HD] = o_scr[hh * RB:(hh + 1) * RB, :].astype(BF16)
            a2a_send(aos, aor, *aosem, j)
        a2a_wait_recv(aos, aor, *aosem)
        put_rows(nbuf, [aor[p].astype(F32) for p in range(ROWS)])

        if layer == 0:
            for j in range(2):
                @pl.when(jnp.logical_not(jnp.logical_and(home, lax.rem(r, 2) == j)))
                def _():
                    pltpu.make_async_remote_copy(xi_send.at[0], xi_recv.at[j], xisem.at[0], xisem.at[1 + j],
                                                 device_id=dev(c, r), device_id_type=MESH).wait_recv()
                xown[:, j * D:(j + 1) * D] = xi_recv[j].astype(F32)

        os_, or_ = o_s.at[layer], o_r.at[layer]
        osem = (rssem.at[layer, 1], rrsem.at[layer, 1])

        def o_body(i, slots):
            lhs = nbuf[...]
            y = [jnp.dot(lhs, wbuf[s], preferred_element_type=F32) for s in slots]
            rs_send(os_, or_, *osem, i * (3 * CW), jnp.concatenate(y, axis=1))

        def residual(send, recv, sems, which):
            rs_wait_recv(recv, *sems)
            xs, xr = x_s.at[layer, which], x_r.at[layer, which]
            xsem = (assem.at[layer, 1 + which], arsem.at[layer, 1 + which])
            squares = jnp.zeros((RB, 128), F32)
            for j in range(2):
                update = rs_sum(send, recv, j * D, (j + 1) * D).astype(BF16).astype(F32)
                x = (xown[:, j * D:(j + 1) * D] + update).astype(BF16)
                xs[j] = x
                x = x.astype(F32)
                xown[:, j * D:(j + 1) * D] = x
                a2a_send(xs, xr, *xsem, j)
                sq = x * x
                for k in range(D // 128):
                    squares = squares + sq[:, k * 128:(k + 1) * 128]
            last = layer == LAYERS - 1 and which == 1
            if not last:
                sts, stv = st_s.at[layer, which], st_r.at[layer, which]
                stat = jnp.broadcast_to(jnp.sum(squares, axis=1, keepdims=True), (RB, 128))
                sts[...] = stat
                stv[me] = stat
                for e in range(1, COLS * ROWS):
                    stat_copy(sts, stv, stsem.at[layer, which, 0], stsem.at[layer, which, 1], e).start()
            a2a_wait_recv(xs, xr, *xsem)
            if last:
                return
            seven = stv.at[pl.ds(0, COLS * ROWS - 1)]
            pltpu.make_async_remote_copy(seven, seven, stsem.at[layer, which, 0], stsem.at[layer, which, 1],
                                         device_id=dev(c, r), device_id_type=MESH).wait_recv()
            g = (gmbuf[layer:layer + 1, :] if which == 0 else gabuf[layer + 1:layer + 2, :]).astype(F32)
            parts = []
            for p in range(ROWS):
                parts.append(normalise(p, xr[p].astype(F32), stv[p] + stv[ROWS + p], g))
            put_rows(nbuf, parts)

        run_phase(layer, BASE['o'], 0, 2, 3, False, o_body)
        residual(os_, or_, osem, 0)

        def gu_cols(i):
            return pl.ds(i * GB if isinstance(i, int) else pl.multiple_of(i * GB, GB), GB)

        def gu_body(i, slots):
            lhs = nbuf[...]
            y = jnp.concatenate([jnp.dot(lhs, wbuf[s], preferred_element_type=F32) for s in slots], axis=1)
            cols = gu_cols(i)
            for p in range(2):
                even, odd = y[2 * p * RB:(2 * p + 1) * RB], y[(2 * p + 1) * RB:(2 * p + 2) * RB]
                gk[p, :, cols] = jnp.where(core == 0, even, odd)
                gd_s[layer, p, :, cols] = jnp.where(core == 0, odd, even).astype(BF16)
            pltpu.make_async_remote_copy(gd_s.at[layer, :, :, cols], gd_r.at[layer, :, :, cols], gdsem.at[layer], gdrem.at[layer, i],
                                         device_id=dev(c, sibling), device_id_type=MESH).start()

            @pl.when(i >= LAG)
            def _():
                pair_sum(i - LAG)

        def pair_sum(i):
            cols = gu_cols(i)
            pltpu.make_async_remote_copy(gd_s.at[layer, :, :, cols], gd_r.at[layer, :, :, cols], gdsem.at[layer], gdrem.at[layer, i],
                                         device_id=dev(c, sibling), device_id_type=MESH).wait_recv()
            s0 = gk[0, :, cols] + gd_r[layer, 0, :, cols].astype(F32)
            s1 = gk[1, :, cols] + gd_r[layer, 1, :, cols].astype(F32)
            gk[0, :, cols] = jnp.where(chip == 0, s0, s1)
            gx_s[layer, :, cols] = jnp.where(chip == 0, s1, s0).astype(BF16)
            pltpu.make_async_remote_copy(gx_s.at[layer, :, cols], gx_r.at[layer, :, cols], gxsem.at[layer], gxrem.at[layer, i // (GT // NP)],
                                         device_id=dev(c, across), device_id_type=MESH).start()

        def activate(q):
            width = GT // NP * GB
            ref = gx_r.at[layer, :, pl.ds(q * width, width)]
            pltpu.make_async_remote_copy(ref, ref, gxsem.at[layer], gxrem.at[layer, q], device_id=dev(c, r), device_id_type=MESH).wait_recv()
            for j in range(2):
                for w in range(2):
                    lo = q * width + (2 * j + w) * 2 * CW
                    mid, hi = lo + CW, lo + 2 * CW
                    gate = (gk[0, :, lo:mid] + gx_r[layer, :, lo:mid].astype(F32)).astype(BF16).astype(F32)
                    up = (gk[0, :, mid:hi] + gx_r[layer, :, mid:hi].astype(F32)).astype(BF16).astype(F32)
                    aa_s[layer, q, j, :, w * CW:(w + 1) * CW] = (gate * jax.nn.sigmoid(gate) * up).astype(BF16)
            act_send(layer, q)

        ds_, dr_ = d_s.at[layer], d_r.at[layer]
        dsem = (rssem.at[layer, 2], rrsem.at[layer, 2])

        def d_part(q):
            def body(i, slots):
                lhs = abuf[:, q * KD:(q + 1) * KD]
                y = [jnp.dot(lhs, wbuf[s, 0:KD], preferred_element_type=F32) for s in slots]
                y = jnp.concatenate(y, axis=1)
                cols = slice(i * 3 * CW, (i + 1) * 3 * CW)
                if q > 0:
                    y = y + dacc[:, cols]
                if q < NP - 1:
                    dacc[:, cols] = y
                else:
                    rs_send(ds_, dr_, *dsem, i * (3 * CW), y)

            act_wait(layer, q)
            abuf[:, q * KD:(q + 1) * KD] = jnp.concatenate([aa_r[layer, q, p].astype(F32) for p in range(ROWS)], axis=0).astype(BF16)
            for i in range(2):
                run_phase(layer, BASE['d'] + q * DN, i, i + 1, 3, True, body)

        run_phase(layer, BASE['gu'], 0, 6, 4, False, gu_body)
        activate(0)
        run_phase(layer, BASE['gu'], 6, GT, 4, False, gu_body)
        activate(1)
        act_relay(layer, 0)
        for i in range(GT - LAG, GT):
            pair_sum(i)
        activate(2)
        act_relay(layer, 1)
        d_part(0)
        activate(3)
        act_relay(layer, 2)
        d_part(1)
        act_relay(layer, 3)
        d_part(2)
        d_part(3)
        residual(ds_, dr_, dsem, 1)

    final = [x_r[LAYERS - 1, 1, p].astype(F32) for p in range(ROWS)]
    out0[...] = jnp.concatenate([f[0:4] for f in final], axis=0).astype(BF16)
    out1[...] = jnp.concatenate([f[4:8] for f in final], axis=0).astype(BF16)

    pltpu.make_async_remote_copy(is_recv, is_recv, isem.at[0], isem.at[1], device_id=dev(c, r), device_id_type=MESH).wait_send()

    @pl.when(home)
    def _():
        three = xi_send.at[pl.ds(0, 3)]
        pltpu.make_async_remote_copy(three, three, xisem.at[0], xisem.at[1], device_id=dev(c, r), device_id_type=MESH).wait_send()

    for layer in range(LAYERS):
        for ph, (send, recv) in enumerate(((qkv_s, qkv_r), (o_s, o_r), (d_s, d_r))):
            rs_wait_send(send.at[layer], rssem.at[layer, ph], rrsem.at[layer, ph])
        for ph, (send, recv) in enumerate(((ao_s.at[layer], ao_r.at[layer]), (x_s.at[layer, 0], x_r.at[layer, 0]),
                                           (x_s.at[layer, 1], x_r.at[layer, 1]))):
            a2a_wait_send(send, recv, assem.at[layer, ph], arsem.at[layer, ph])
        pltpu.make_async_remote_copy(gd_s.at[layer], gd_s.at[layer], gdsem.at[layer], gdrem.at[layer, 0], device_id=dev(c, r), device_id_type=MESH).wait_send()
        pltpu.make_async_remote_copy(gx_s.at[layer], gx_s.at[layer], gxsem.at[layer], gxrem.at[layer, 0], device_id=dev(c, r), device_id_type=MESH).wait_send()
        for h in range(NP):
            act_wait_send(layer, h)
        for which in range(2):
            if layer == LAYERS - 1 and which == 1:
                continue
            seven = st_r.at[layer, which, pl.ds(0, COLS * ROWS - 1)]
            pltpu.make_async_remote_copy(seven, seven, stsem.at[layer, which, 0], stsem.at[layer, which, 1],
                                         device_id=dev(c, r), device_id_type=MESH).wait_send()


def solution(mesh):
    hidden_spec = P('rep', 'row')
    index_spec = P(('rep', 'row'))
    cache_spec = P(None, ('rep', 'row'), None, 'col', None)
    gain_spec = P(None, 'row')
    weight_spec = P(None, 'row', 'col')

    def device_program(hidden_0, hidden_1, positions, lengths, cache_k, cache_v, norm_attn, norm_mlp,
                       w_query, w_key, w_value, w_out, w_gate, w_up, w_down):
        cache_shape = cache_k.shape
        flat = (LAYERS, SEQS, CTX * KVH, HD)
        any_spec = pl.BlockSpec(memory_space=pl.ANY)
        smem = pl.BlockSpec(memory_space=pltpu.SMEM)
        vmem = pl.BlockSpec(memory_space=pltpu.VMEM)
        V = pltpu.VMEM
        DMA = pltpu.SemaphoreType.DMA
        scratch = [
            V((NS, D, CW), BF16), V((2, 16, D), BF16),
            V((LAYERS, D), BF16), V((LAYERS, D), BF16), V((ROWS * RB, D), BF16), V((ROWS * RB, FK), BF16), V((RB, QW), F32),
            V((QH * RB, HD), F32), V((KVH * RB, HD), F32), V((KVH * RB, HD), F32), V((QH * RB, HD), F32),
            V((2 * QH, CTX * KVH), jnp.int32), V((RB, HD), F32), V((RB, HD), F32),
            V((ROWS, RB, 128), F32), V((3, ROWS, RB, 128), F32), V((ROWS, RB, D), BF16), V((2, RB, D), BF16),
            V((LAYERS, ROWS, RB, QKV_N), BF16), V((LAYERS, 3, RB, QKV_N), BF16),
            V((LAYERS, ROWS, RB, QW), BF16), V((LAYERS, 3, RB, QW), BF16),
            V((LAYERS, 2, RB, 2 * FF), BF16), V((LAYERS, 2, RB, 2 * FF), BF16), V((2, RB, 2 * FF), F32),
            V((LAYERS, RB, 2 * FF), BF16), V((LAYERS, RB, 2 * FF), BF16),
            V((LAYERS, ROWS, RB, QW), BF16), V((LAYERS, 3, RB, QW), BF16), V((ROWS * RB, QW), F32),
            V((LAYERS, 2, RB, D), BF16), V((LAYERS, ROWS, RB, D), BF16),
            V((LAYERS, 2, 2, RB, D), BF16), V((LAYERS, 2, ROWS, RB, D), BF16),
            V((LAYERS, NP, 2, RB, KD), BF16), V((LAYERS, NP, ROWS, RB, KD), BF16), V((LAYERS, NP, 2, RB, KD), BF16),
            V((LAYERS, 2, RB, 128), F32), V((LAYERS, 2, COLS * ROWS, RB, 128), F32),
            DMA((NS,)), DMA((6,)), DMA((2,)), DMA((3,)),
            DMA((LAYERS, 3)), DMA((LAYERS, 3)), DMA((LAYERS, 3, 4)), DMA((LAYERS, 3, 4)), DMA((LAYERS, 2, 2)),
            DMA((LAYERS,)), DMA((LAYERS, GT)), DMA((LAYERS,)), DMA((LAYERS, NP)), DMA((LAYERS, NP, 7)), DMA((LAYERS, NP, 5)),
        ]
        shapes = (hidden_0.shape, hidden_1.shape, flat, flat)
        results = tuple(V(shape, BF16) for shape in shapes)
        out = pl.pallas_call(
            mega_kernel,
            out_shape=results,
            in_specs=[any_spec, any_spec, smem, smem] + [any_spec] * 11,
            out_specs=(vmem,) * 4,
            scratch_shapes=scratch,
            compiler_params=pltpu.CompilerParams(collective_id=0, has_side_effects=True, vmem_limit_bytes=63000000),
        )(hidden_0, hidden_1, positions, lengths, cache_k.reshape(flat), cache_v.reshape(flat), norm_attn, norm_mlp,
          w_query, w_key, w_value, w_out, w_gate, w_up, w_down)
        return out[0], out[1], out[2].reshape(cache_shape), out[3].reshape(cache_shape)

    return jax.shard_map(device_program, mesh=mesh,
                         in_specs=(hidden_spec, hidden_spec, index_spec, index_spec, cache_spec, cache_spec, gain_spec, gain_spec) + (weight_spec,) * 7,
                         out_specs=(hidden_spec, hidden_spec, cache_spec, cache_spec), check_vma=False)
```

```python
import functools

import jax
import jax.numpy as jnp
from jax import lax
from jax.experimental import pallas as pl
from jax.experimental.pallas import tpu as pltpu
from jax.sharding import PartitionSpec as P

ROPE_BASE = 1000000.0
EPS = 1e-05
MESH = pl.DeviceIdType.MESH
F32 = jnp.float32
BF16 = jnp.bfloat16

LAYERS = 2
ROWS = 4
COLS = 2
SEQS = 4
RB = 8
D = 1536
HD = 128
QH = 24
KVH = 4
QW = QH * HD
KVW = KVH * HD
FF = 8192
FK = 4096
WIDTH = 6144
CTX = 128
CW = 512
KD = 1024
NS = 30

QKV_N = QW + 2 * KVW
KINDS = ['k', 'v'] + ['q'] * 6 + ['o'] * 6 + ['g', 'u'] * 16 + ['d'] * 24
INDEX = [0, 0] + list(range(6)) + list(range(6)) + [i // 2 for i in range(32)] + list(range(24))
PER_LAYER = len(KINDS)
TOTAL = LAYERS * PER_LAYER
BASE = {'qkv': 0, 'o': 8, 'gu': 14, 'd': 46}
NP = 4
DN = 6
GT = 8
GB = 4 * CW
LAG = 1
RELAYED = (1,)


def chunk_of(seq):
    if seq >= TOTAL:
        return None
    layer, pos = divmod(seq, PER_LAYER)
    return layer, KINDS[pos], INDEX[pos]


def mega_kernel(h0, h1, positions, lengths, ck, cv, na, nm, wq, wk, wv, wo, wg, wu, wd,
                out0, out1, kbuf, vbuf,
                wbuf, hbuf, gabuf, gmbuf, nbuf, abuf, xown,
                q_scr, kn_scr, vn_scr, o_scr, lim_scr, cos_scr, sin_scr,
                is_send, is_recv, xi_send, xi_recv,
                qkv_s, qkv_r, o_s, o_r, gd_s, gd_r, gk, gx_s, gx_r, d_s, d_r, dacc,
                ao_s, ao_r, x_s, x_r, aa_s, aa_r, aa_m, st_s, st_r,
                wsem, lsem, isem, xisem, rssem, rrsem, assem, arsem, stsem, gdsem, gdrem, gxsem, gxrem, acsem, acrem):
    c = lax.axis_index('col')
    r = lax.axis_index('row')
    rep = lax.axis_index('rep')
    me = c * ROWS + r
    home = c == r // 2

    def dev(cc, rr):
        return (rep, cc, rr)

    small = [pltpu.make_async_copy(h0, hbuf.at[0], lsem.at[0]),
             pltpu.make_async_copy(h1, hbuf.at[1], lsem.at[1]),
             pltpu.make_async_copy(na, gabuf, lsem.at[2]),
             pltpu.make_async_copy(nm, gmbuf, lsem.at[3]),
             pltpu.make_async_copy(ck, kbuf, lsem.at[4]),
             pltpu.make_async_copy(cv, vbuf, lsem.at[5])]
    for copy in small[:4]:
        copy.start()

    def weight_copy(layer, kind, idx, slot):
        if kind == 'd':
            k, n = idx // DN, idx % DN
            src = wd.at[layer, pl.ds(pl.multiple_of(k * KD, KD), KD), pl.ds(pl.multiple_of(n * CW, CW), CW)]
            return pltpu.make_async_copy(src, wbuf.at[slot, pl.ds(0, KD)], wsem.at[slot])
        ref = {'k': wk, 'v': wv, 'q': wq, 'o': wo, 'g': wg, 'u': wu}[kind]
        if kind in 'gu':
            idx = 8 * ((idx % 4) // 2) + 2 * (idx // 4) + idx % 2
        src = ref.at[layer, :, pl.ds(pl.multiple_of(idx * CW, CW), CW)]
        return pltpu.make_async_copy(src, wbuf.at[slot], wsem.at[slot])

    def weight_wait(down, slot):
        if down:
            pltpu.make_async_copy(wd.at[0, pl.ds(0, KD), pl.ds(0, CW)], wbuf.at[slot, pl.ds(0, KD)], wsem.at[slot]).wait()
        else:
            pltpu.make_async_copy(wq.at[0, :, pl.ds(0, CW)], wbuf.at[slot], wsem.at[slot]).wait()

    def issue_initial(lo, hi):
        seq = lo
        while seq < hi:
            layer, kind, idx = chunk_of(seq)
            weight_copy(layer, kind, idx, seq % NS).start(priority=1)
            seq += 1

    issue_initial(0, 8)
    for copy in small[4:]:
        copy.start()
    issue_initial(8, NS)

    def run_phase(layer, base, lo, iters, per, down, body):
        start = layer * PER_LAYER + base

        def future(t):
            return [chunk_of(start + t * per + e + NS) for e in range(per)]

        def signature(t):
            return [None if f is None else f[:2] for f in future(t)]

        t = lo
        while t < iters:
            end = t + 1
            while end < iters and signature(end) == signature(t):
                end += 1
            first = future(t)
            step = [0] * per
            if end - t > 1:
                nxt = future(t + 1)
                step = [0 if f is None else g[2] - f[2] for f, g in zip(first, nxt)]
                for tt in range(t, end):
                    for f, s, g in zip(first, step, future(tt)):
                        assert f is None or f[2] + s * (tt - t) == g[2]

            def one(i, carry, t=t, first=first, step=step):
                slots = [lax.rem(start + i * per + e, NS) for e in range(per)]
                for s in slots:
                    weight_wait(down, s)
                body(i, slots)
                for f, st, s in zip(first, step, slots):
                    if f is not None:
                        weight_copy(f[0], f[1], f[2] + st * (i - t), s).start(priority=1)
                return carry

            if end - t == 1:
                one(t, 0)
            else:
                lax.fori_loop(t, end, one, 0)
            t = end

    def rs_send(send, recv, ssem, rsem, off, value):
        width = value.shape[1]
        cols = pl.ds(off if isinstance(off, int) else pl.multiple_of(off, width), width)
        for p in range(ROWS):
            send[p, :, cols] = value[p * RB:(p + 1) * RB].astype(BF16)
        for d in (2, 3, 1):
            tgt = lax.rem(r + d, ROWS)
            pltpu.make_async_remote_copy(send.at[tgt, :, cols], recv.at[d - 1, :, cols], ssem, rsem,
                                         device_id=dev(c, tgt), device_id_type=MESH).start()

    def rs_wait_recv(recv, ssem, rsem):
        pltpu.make_async_remote_copy(recv, recv, ssem, rsem, device_id=dev(c, r), device_id_type=MESH).wait_recv()

    def rs_wait_send(send, ssem, rsem):
        ref = send.at[pl.ds(0, 3)]
        pltpu.make_async_remote_copy(ref, ref, ssem, rsem, device_id=dev(c, r), device_id_type=MESH).wait_send()

    def rs_sum(send, recv, lo, hi):
        acc = send[r, :, lo:hi].astype(F32)
        for d in range(ROWS - 1):
            acc = acc + recv[d, :, lo:hi].astype(F32)
        return acc

    def a2a_copy(send, recv, ssem, rsem, j, cc):
        return pltpu.make_async_remote_copy(send.at[j], recv.at[r], ssem.at[j * COLS + cc], rsem.at[r],
                                            device_id=dev(cc, 2 * c + j), device_id_type=MESH)

    def a2a_self(j, cc):
        return jnp.logical_and(c == cc, r == 2 * c + j)

    def a2a_send(send, recv, ssem, rsem, j):
        for cc in range(COLS):
            mine = a2a_self(j, cc)

            @pl.when(jnp.logical_not(mine))
            def _():
                a2a_copy(send, recv, ssem, rsem, j, cc).start()

            @pl.when(mine)
            def _():
                recv[r] = send[j]

    def a2a_wait_recv(send, recv, ssem, rsem):
        for s in range(ROWS):
            @pl.when(jnp.logical_not(jnp.logical_and(home, r == s)))
            def _():
                pltpu.make_async_remote_copy(send.at[0], recv.at[s], ssem.at[0], rsem.at[s],
                                             device_id=dev(c, r), device_id_type=MESH).wait_recv()

    def a2a_wait_send(send, recv, ssem, rsem):
        for j in range(2):
            for cc in range(COLS):
                @pl.when(jnp.logical_not(a2a_self(j, cc)))
                def _():
                    a2a_copy(send, recv, ssem, rsem, j, cc).wait_send()

    core, chip = lax.rem(r, 2), r // 2
    sibling = r + 1 - 2 * core
    across = 2 * (1 - chip) + core

    def act_near(layer, h, j):
        return pltpu.make_async_remote_copy(aa_s.at[layer, h, j], aa_r.at[layer, h, r], acsem.at[layer, h, j], acrem.at[layer, h, r],
                                            device_id=dev(c, 2 * c + j), device_id_type=MESH)

    def act_far(layer, h, j):
        return pltpu.make_async_remote_copy(aa_s.at[layer, h, j], aa_r.at[layer, h, r], acsem.at[layer, h, 2 + j], acrem.at[layer, h, r],
                                            device_id=dev(1 - c, 2 * c + j), device_id_type=MESH)

    def act_hand(layer, h):
        return pltpu.make_async_remote_copy(aa_s.at[layer, h], aa_m.at[layer, h], acsem.at[layer, h, 4], acrem.at[layer, h, 4],
                                            device_id=dev(1 - c, r), device_id_type=MESH)

    def act_forward(layer, h, j):
        return pltpu.make_async_remote_copy(aa_m.at[layer, h, j], aa_r.at[layer, h, r], acsem.at[layer, h, 5 + j], acrem.at[layer, h, r],
                                            device_id=dev(c, 2 * (1 - c) + j), device_id_type=MESH)

    def act_diag(layer, h, j):
        return pltpu.make_async_remote_copy(aa_s.at[layer, h, j], aa_r.at[layer, h, r], acsem.at[layer, h, 2 + j], acrem.at[layer, h, r],
                                            device_id=dev(1 - c, 2 * c + j), device_id_type=MESH)

    def act_send(layer, h):
        @pl.when(jnp.logical_not(home))
        def _():
            if h in RELAYED:
                act_hand(layer, h).start()
            else:
                for j in range(2):
                    act_diag(layer, h, j).start()
            for j in range(2):
                act_near(layer, h, j).start()

        @pl.when(home)
        def _():
            for j in range(2):
                act_far(layer, h, j).start()
            for j in range(2):
                @pl.when(core != j)
                def _():
                    act_near(layer, h, j).start()

                @pl.when(core == j)
                def _():
                    aa_r[layer, h, r] = aa_s[layer, h, j]

    def act_relay(layer, h):
        if h not in RELAYED:
            return

        @pl.when(home)
        def _():
            act_hand(layer, h).wait_recv()
            for j in range(2):
                act_forward(layer, h, j).start()

    def act_wait(layer, h):
        for s in range(ROWS):
            @pl.when(jnp.logical_not(jnp.logical_and(home, r == s)))
            def _():
                pltpu.make_async_remote_copy(aa_s.at[layer, h, 0], aa_r.at[layer, h, s], acsem.at[layer, h, 0], acrem.at[layer, h, s],
                                             device_id=dev(c, r), device_id_type=MESH).wait_recv()

    def act_wait_send(layer, h):
        @pl.when(jnp.logical_not(home))
        def _():
            if h in RELAYED:
                act_hand(layer, h).wait_send()
            else:
                for j in range(2):
                    act_diag(layer, h, j).wait_send()
            for j in range(2):
                act_near(layer, h, j).wait_send()

        @pl.when(home)
        def _():
            for j in range(2):
                act_far(layer, h, j).wait_send()
                if h in RELAYED:
                    act_forward(layer, h, j).wait_send()

                @pl.when(core != j)
                def _():
                    act_near(layer, h, j).wait_send()

    def stat_copy(send, recv, ssem, rsem, e):
        tgt = lax.rem(me + e, COLS * ROWS)
        return pltpu.make_async_remote_copy(send, recv.at[me], ssem, rsem,
                                            device_id=dev(tgt // ROWS, lax.rem(tgt, ROWS)), device_id_type=MESH)

    barrier = pltpu.get_barrier_semaphore()
    for e in range(1, COLS * ROWS):
        tgt = lax.rem(me + e, COLS * ROWS)
        pl.semaphore_signal(barrier, inc=1, device_id=dev(tgt // ROWS, lax.rem(tgt, ROWS)), device_id_type=MESH)
    pl.semaphore_wait(barrier, COLS * ROWS - 1)

    for copy in small[:4]:
        copy.wait()
    h0v = hbuf[0].astype(F32)
    h1v = hbuf[1].astype(F32)
    blocks = [jnp.concatenate([h0v[4 * p:4 * p + 4], h1v[4 * p:4 * p + 4]], axis=0) for p in range(ROWS)]
    for p in range(ROWS):
        sq = jnp.sum(blocks[p] * blocks[p], axis=1, keepdims=True)
        is_send[p] = jnp.broadcast_to(sq, (RB, 128))
    for d in (2, 3, 1):
        tgt = lax.rem(r + d, ROWS)
        pltpu.make_async_remote_copy(is_send, is_recv.at[d - 1], isem.at[0], isem.at[1],
                                     device_id=dev(c, tgt), device_id_type=MESH).start()
    for p in range(ROWS):
        xi_send[p] = blocks[p].astype(BF16)

    @pl.when(home)
    def _():
        for d in range(1, ROWS):
            tgt = lax.rem(r + d, ROWS)
            pltpu.make_async_remote_copy(xi_send.at[tgt], xi_recv.at[lax.rem(r, 2)], xisem.at[0], xisem.at[1 + lax.rem(r, 2)],
                                         device_id=dev(c, tgt), device_id_type=MESH).start()
        xi_recv[lax.rem(r, 2)] = xi_send[r]

    rowi = lax.broadcasted_iota(jnp.int32, (RB, HD), 0)
    lane = lax.broadcasted_iota(jnp.int32, (RB, HD), 1)
    step_id = (rowi >= SEQS).astype(jnp.int32)
    seq_id = rowi - SEQS * step_id
    pos = step_id
    for b in range(SEQS):
        pos = pos + jnp.where(seq_id == b, positions[b], 0)
    half = (lane >= HD // 2)
    freq_i = jnp.where(half, lane - HD // 2, lane).astype(F32)
    inv_freq = jnp.exp(freq_i * (-13.815510557964274 / 64.0))
    angle = pos.astype(F32) * inv_freq
    cos_scr[...] = jnp.cos(angle)
    sine = jnp.sin(angle)
    sin_scr[...] = jnp.where(half, sine, -sine)

    srow = lax.broadcasted_iota(jnp.int32, (2 * QH, CTX * KVH), 0)
    scol = lax.broadcasted_iota(jnp.int32, (2 * QH, CTX * KVH), 1)
    srow_step = (srow >= QH).astype(jnp.int32)
    srow_h = srow - QH * srow_step
    srow_kv = (srow_h >= 6).astype(jnp.int32) + (srow_h >= 12).astype(jnp.int32) + (srow_h >= 18).astype(jnp.int32)
    slot = jnp.right_shift(scol, 2)
    kv_of = jnp.bitwise_and(scol, 3)
    lim_scr[...] = jnp.where(kv_of == srow_kv, slot - srow_step, 1 << 20)

    pltpu.make_async_remote_copy(is_recv, is_recv, isem.at[0], isem.at[1], device_id=dev(c, r), device_id_type=MESH).wait_recv()

    def normalise(p, xblock, total, gain):
        scale = lax.rsqrt(total * (1.0 / WIDTH) + EPS)[:, :1]
        return xblock * scale * gain

    def put_rows(dst, parts):
        dst[...] = jnp.concatenate(parts, axis=0).astype(BF16)

    gain = gabuf[0:1, :].astype(F32)
    parts = []
    for p in range(ROWS):
        total = is_send[p] + is_recv[0, p] + is_recv[1, p] + is_recv[2, p]
        parts.append(normalise(p, blocks[p], total, gain))
    put_rows(nbuf, parts)

    for copy in small[4:]:
        copy.wait()

    for layer in range(LAYERS):
        qs, qr = qkv_s.at[layer], qkv_r.at[layer]
        qsem = (rssem.at[layer, 0], rrsem.at[layer, 0])

        def lhs_dots(slots):
            lhs = nbuf[...]
            return jnp.concatenate([jnp.dot(lhs, wbuf[s], preferred_element_type=F32) for s in slots], axis=1)

        early = 4 * CW

        def qkv_first(i, slots):
            rs_send(qs, qr, qsem[0], rrsem.at[layer, 3], 0, lhs_dots(slots))

        def qkv_rest(i, slots):
            off = i * (2 * CW) + early
            rs_send(qs, qr, *qsem, off, lhs_dots(slots))

        run_phase(layer, BASE['qkv'], 0, 1, 4, False, qkv_first)
        run_phase(layer, BASE['qkv'] + 4, 0, 2, 2, False, qkv_rest)
        part = qr.at[:, :, pl.ds(0, early)]
        pltpu.make_async_remote_copy(part, part, qsem[0], rrsem.at[layer, 3], device_id=dev(c, r), device_id_type=MESH).wait_recv()

        cosv, sinv = cos_scr[...], sin_scr[...]

        def rope(block):
            value = block.astype(BF16).astype(F32)
            return (value * cosv + pltpu.roll(value, HD // 2, 1) * sinv).astype(BF16).astype(F32)

        for h in range(KVH):
            kn_scr[h * RB:(h + 1) * RB, :] = rope(rs_sum(qs, qr, h * HD, (h + 1) * HD))
            vn_scr[h * RB:(h + 1) * RB, :] = rs_sum(qs, qr, KVW + h * HD, KVW + (h + 1) * HD)
        def query(lo, hi):
            for h in range(lo, hi):
                q_scr[h * RB:(h + 1) * RB, :] = rope(rs_sum(qs, qr, 2 * KVW + h * HD, 2 * KVW + (h + 1) * HD))

        query(0, 8)
        row_slot = jnp.right_shift(lax.broadcasted_iota(jnp.int32, (CTX * KVH, HD), 0), 2)
        for b in range(SEQS):
            length = lengths[b]

            def updated(cache, new_scr):
                value = cache[layer, b].astype(F32)
                for s in range(2):
                    new = new_scr[pl.ds(b + SEQS * s, KVH, stride=RB), :]
                    tile = jnp.concatenate([new, new], axis=0)
                    full = jnp.broadcast_to(tile[None], (CTX * KVH // 8, 8, HD)).reshape(CTX * KVH, HD)
                    value = jnp.where(row_slot == length + s, full, value)
                return value.astype(BF16)

            kbuf[layer, b] = updated(kbuf, kn_scr)
            vbuf[layer, b] = updated(vbuf, vn_scr)

        part = qr.at[:, :, pl.ds(early, QKV_N - early)]
        pltpu.make_async_remote_copy(part, part, *qsem, device_id=dev(c, r), device_id_type=MESH).wait_recv()
        query(8, QH)
        scores = []
        for b in range(SEQS):
            qb = jnp.concatenate([q_scr[pl.ds(b + SEQS * s, QH, stride=RB), :] for s in range(2)], axis=0).astype(BF16)
            scores.append(lax.dot_general(qb, kbuf[layer, b], (((1,), (1,)), ((), ())), preferred_element_type=F32))
        probs = []
        for b in range(SEQS):
            sc = jnp.where(lim_scr[...] <= lengths[b], scores[b] * (HD ** -0.5), -jnp.inf)
            e = jnp.exp(sc - jnp.max(sc, axis=1, keepdims=True))
            probs.append((e / jnp.sum(e, axis=1, keepdims=True)).astype(BF16))
        outs = [jnp.dot(probs[b], vbuf[layer, b], preferred_element_type=F32) for b in range(SEQS)]
        for b in range(SEQS):
            for s in range(2):
                o_scr[pl.ds(b + SEQS * s, QH, stride=RB), :] = outs[b][s * QH:(s + 1) * QH]
        aos, aor = ao_s.at[layer], ao_r.at[layer]
        aosem = (assem.at[layer, 0], arsem.at[layer, 0])
        for j in range(2):
            for h in range(QH // 2):
                hh = j * (QH // 2) + h
                aos[j, :, h * HD:(h + 1) * HD] = o_scr[hh * RB:(hh + 1) * RB, :].astype(BF16)
            a2a_send(aos, aor, *aosem, j)
        a2a_wait_recv(aos, aor, *aosem)
        put_rows(nbuf, [aor[p].astype(F32) for p in range(ROWS)])

        if layer == 0:
            for j in range(2):
                @pl.when(jnp.logical_not(jnp.logical_and(home, lax.rem(r, 2) == j)))
                def _():
                    pltpu.make_async_remote_copy(xi_send.at[0], xi_recv.at[j], xisem.at[0], xisem.at[1 + j],
                                                 device_id=dev(c, r), device_id_type=MESH).wait_recv()
                xown[:, j * D:(j + 1) * D] = xi_recv[j].astype(F32)

        os_, or_ = o_s.at[layer], o_r.at[layer]
        osem = (rssem.at[layer, 1], rrsem.at[layer, 1])

        def o_body(i, slots):
            lhs = nbuf[...]
            y = [jnp.dot(lhs, wbuf[s], preferred_element_type=F32) for s in slots]
            rs_send(os_, or_, *osem, i * (2 * CW), jnp.concatenate(y, axis=1))

        def residual(send, recv, sems, which):
            rs_wait_recv(recv, *sems)
            xs, xr = x_s.at[layer, which], x_r.at[layer, which]
            xsem = (assem.at[layer, 1 + which], arsem.at[layer, 1 + which])
            squares = jnp.zeros((RB, 128), F32)
            for j in range(2):
                update = rs_sum(send, recv, j * D, (j + 1) * D).astype(BF16).astype(F32)
                x = (xown[:, j * D:(j + 1) * D] + update).astype(BF16)
                xs[j] = x
                x = x.astype(F32)
                xown[:, j * D:(j + 1) * D] = x
                a2a_send(xs, xr, *xsem, j)
                sq = x * x
                for k in range(D // 128):
                    squares = squares + sq[:, k * 128:(k + 1) * 128]
            last = layer == LAYERS - 1 and which == 1
            if not last:
                sts, stv = st_s.at[layer, which], st_r.at[layer, which]
                stat = jnp.broadcast_to(jnp.sum(squares, axis=1, keepdims=True), (RB, 128))
                sts[...] = stat
                stv[me] = stat
                for e in range(1, COLS * ROWS):
                    stat_copy(sts, stv, stsem.at[layer, which, 0], stsem.at[layer, which, 1], e).start()
            a2a_wait_recv(xs, xr, *xsem)
            if last:
                return
            seven = stv.at[pl.ds(0, COLS * ROWS - 1)]
            pltpu.make_async_remote_copy(seven, seven, stsem.at[layer, which, 0], stsem.at[layer, which, 1],
                                         device_id=dev(c, r), device_id_type=MESH).wait_recv()
            g = (gmbuf[layer:layer + 1, :] if which == 0 else gabuf[layer + 1:layer + 2, :]).astype(F32)
            parts = []
            for p in range(ROWS):
                parts.append(normalise(p, xr[p].astype(F32), stv[p] + stv[ROWS + p], g))
            put_rows(nbuf, parts)

        run_phase(layer, BASE['o'], 0, 3, 2, False, o_body)
        residual(os_, or_, osem, 0)

        def gu_cols(i):
            return pl.ds(i * GB if isinstance(i, int) else pl.multiple_of(i * GB, GB), GB)

        def gu_body(i, slots):
            lhs = nbuf[...]
            y = jnp.concatenate([jnp.dot(lhs, wbuf[s], preferred_element_type=F32) for s in slots], axis=1)
            cols = gu_cols(i)
            for p in range(2):
                even, odd = y[2 * p * RB:(2 * p + 1) * RB], y[(2 * p + 1) * RB:(2 * p + 2) * RB]
                gk[p, :, cols] = jnp.where(core == 0, even, odd)
                gd_s[layer, p, :, cols] = jnp.where(core == 0, odd, even).astype(BF16)
            pltpu.make_async_remote_copy(gd_s.at[layer, :, :, cols], gd_r.at[layer, :, :, cols], gdsem.at[layer], gdrem.at[layer, i],
                                         device_id=dev(c, sibling), device_id_type=MESH).start()

            @pl.when(i >= LAG)
            def _():
                pair_sum(i - LAG)

        def pair_sum(i):
            cols = gu_cols(i)
            pltpu.make_async_remote_copy(gd_s.at[layer, :, :, cols], gd_r.at[layer, :, :, cols], gdsem.at[layer], gdrem.at[layer, i],
                                         device_id=dev(c, sibling), device_id_type=MESH).wait_recv()
            s0 = gk[0, :, cols] + gd_r[layer, 0, :, cols].astype(F32)
            s1 = gk[1, :, cols] + gd_r[layer, 1, :, cols].astype(F32)
            gk[0, :, cols] = jnp.where(chip == 0, s0, s1)
            gx_s[layer, :, cols] = jnp.where(chip == 0, s1, s0).astype(BF16)
            pltpu.make_async_remote_copy(gx_s.at[layer, :, cols], gx_r.at[layer, :, cols], gxsem.at[layer], gxrem.at[layer, i // (GT // NP)],
                                         device_id=dev(c, across), device_id_type=MESH).start()

        def activate(q):
            width = GT // NP * GB
            ref = gx_r.at[layer, :, pl.ds(q * width, width)]
            pltpu.make_async_remote_copy(ref, ref, gxsem.at[layer], gxrem.at[layer, q], device_id=dev(c, r), device_id_type=MESH).wait_recv()
            for j in range(2):
                for w in range(2):
                    lo = q * width + (2 * j + w) * 2 * CW
                    mid, hi = lo + CW, lo + 2 * CW
                    gate = (gk[0, :, lo:mid] + gx_r[layer, :, lo:mid].astype(F32)).astype(BF16).astype(F32)
                    up = (gk[0, :, mid:hi] + gx_r[layer, :, mid:hi].astype(F32)).astype(BF16).astype(F32)
                    aa_s[layer, q, j, :, w * CW:(w + 1) * CW] = (gate * jax.nn.sigmoid(gate) * up).astype(BF16)
            act_send(layer, q)

        ds_, dr_ = d_s.at[layer], d_r.at[layer]
        dsem = (rssem.at[layer, 2], rrsem.at[layer, 2])

        def d_part(q):
            def body(first):
                def run(i, slots):
                    lhs = abuf[:, q * KD:(q + 1) * KD]
                    y = jnp.concatenate([jnp.dot(lhs, wbuf[s, 0:KD], preferred_element_type=F32) for s in slots], axis=1)
                    lo, hi = first * CW, (first + len(slots)) * CW
                    if q > 0:
                        y = y + dacc[:, lo:hi]
                    if q < NP - 1:
                        dacc[:, lo:hi] = y
                        return
                    for part in range(lo, hi, 2 * CW):
                        rs_send(ds_, dr_, *dsem, part, y[:, part - lo:part - lo + 2 * CW])
                return run

            act_wait(layer, q)
            abuf[:, q * KD:(q + 1) * KD] = jnp.concatenate([aa_r[layer, q, p].astype(F32) for p in range(ROWS)], axis=0).astype(BF16)
            for first, count in (((0, DN),) if q < NP - 1 else ((0, 4), (4, 2))):
                run_phase(layer, BASE['d'] + q * DN + first, 0, 1, count, True, body(first))

        run_phase(layer, BASE['gu'], 0, 6, 4, False, gu_body)
        activate(0)
        run_phase(layer, BASE['gu'], 6, GT, 4, False, gu_body)
        activate(1)
        act_relay(layer, 0)
        for i in range(GT - LAG, GT):
            pair_sum(i)
        activate(2)
        act_relay(layer, 1)
        d_part(0)
        activate(3)
        act_relay(layer, 2)
        d_part(1)
        act_relay(layer, 3)
        d_part(2)
        d_part(3)
        residual(ds_, dr_, dsem, 1)

    final = [x_r[LAYERS - 1, 1, p].astype(F32) for p in range(ROWS)]
    out0[...] = jnp.concatenate([f[0:4] for f in final], axis=0).astype(BF16)
    out1[...] = jnp.concatenate([f[4:8] for f in final], axis=0).astype(BF16)

    pltpu.make_async_remote_copy(is_recv, is_recv, isem.at[0], isem.at[1], device_id=dev(c, r), device_id_type=MESH).wait_send()

    @pl.when(home)
    def _():
        three = xi_send.at[pl.ds(0, 3)]
        pltpu.make_async_remote_copy(three, three, xisem.at[0], xisem.at[1], device_id=dev(c, r), device_id_type=MESH).wait_send()

    for layer in range(LAYERS):
        for ph, (send, recv) in enumerate(((qkv_s, qkv_r), (o_s, o_r), (d_s, d_r))):
            rs_wait_send(send.at[layer], rssem.at[layer, ph], rrsem.at[layer, ph])
        for ph, (send, recv) in enumerate(((ao_s.at[layer], ao_r.at[layer]), (x_s.at[layer, 0], x_r.at[layer, 0]),
                                           (x_s.at[layer, 1], x_r.at[layer, 1]))):
            a2a_wait_send(send, recv, assem.at[layer, ph], arsem.at[layer, ph])
        pltpu.make_async_remote_copy(gd_s.at[layer], gd_s.at[layer], gdsem.at[layer], gdrem.at[layer, 0], device_id=dev(c, r), device_id_type=MESH).wait_send()
        pltpu.make_async_remote_copy(gx_s.at[layer], gx_s.at[layer], gxsem.at[layer], gxrem.at[layer, 0], device_id=dev(c, r), device_id_type=MESH).wait_send()
        for h in range(NP):
            act_wait_send(layer, h)
        for which in range(2):
            if layer == LAYERS - 1 and which == 1:
                continue
            seven = st_r.at[layer, which, pl.ds(0, COLS * ROWS - 1)]
            pltpu.make_async_remote_copy(seven, seven, stsem.at[layer, which, 0], stsem.at[layer, which, 1],
                                         device_id=dev(c, r), device_id_type=MESH).wait_send()


def solution(mesh):
    hidden_spec = P('rep', 'row')
    index_spec = P(('rep', 'row'))
    cache_spec = P(None, ('rep', 'row'), None, 'col', None)
    gain_spec = P(None, 'row')
    weight_spec = P(None, 'row', 'col')

    def device_program(hidden_0, hidden_1, positions, lengths, cache_k, cache_v, norm_attn, norm_mlp,
                       w_query, w_key, w_value, w_out, w_gate, w_up, w_down):
        cache_shape = cache_k.shape
        flat = (LAYERS, SEQS, CTX * KVH, HD)
        any_spec = pl.BlockSpec(memory_space=pl.ANY)
        smem = pl.BlockSpec(memory_space=pltpu.SMEM)
        vmem = pl.BlockSpec(memory_space=pltpu.VMEM)
        V = pltpu.VMEM
        DMA = pltpu.SemaphoreType.DMA
        scratch = [
            V((NS, D, CW), BF16), V((2, 16, D), BF16),
            V((LAYERS, D), BF16), V((LAYERS, D), BF16), V((ROWS * RB, D), BF16), V((ROWS * RB, FK), BF16), V((RB, QW), F32),
            V((QH * RB, HD), F32), V((KVH * RB, HD), F32), V((KVH * RB, HD), F32), V((QH * RB, HD), F32),
            V((2 * QH, CTX * KVH), jnp.int32), V((RB, HD), F32), V((RB, HD), F32),
            V((ROWS, RB, 128), F32), V((3, ROWS, RB, 128), F32), V((ROWS, RB, D), BF16), V((2, RB, D), BF16),
            V((LAYERS, ROWS, RB, QKV_N), BF16), V((LAYERS, 3, RB, QKV_N), BF16),
            V((LAYERS, ROWS, RB, QW), BF16), V((LAYERS, 3, RB, QW), BF16),
            V((LAYERS, 2, RB, 2 * FF), BF16), V((LAYERS, 2, RB, 2 * FF), BF16), V((2, RB, 2 * FF), F32),
            V((LAYERS, RB, 2 * FF), BF16), V((LAYERS, RB, 2 * FF), BF16),
            V((LAYERS, ROWS, RB, QW), BF16), V((LAYERS, 3, RB, QW), BF16), V((ROWS * RB, QW), F32),
            V((LAYERS, 2, RB, D), BF16), V((LAYERS, ROWS, RB, D), BF16),
            V((LAYERS, 2, 2, RB, D), BF16), V((LAYERS, 2, ROWS, RB, D), BF16),
            V((LAYERS, NP, 2, RB, KD), BF16), V((LAYERS, NP, ROWS, RB, KD), BF16), V((LAYERS, NP, 2, RB, KD), BF16),
            V((LAYERS, 2, RB, 128), F32), V((LAYERS, 2, COLS * ROWS, RB, 128), F32),
            DMA((NS,)), DMA((6,)), DMA((2,)), DMA((3,)),
            DMA((LAYERS, 3)), DMA((LAYERS, 4)), DMA((LAYERS, 3, 4)), DMA((LAYERS, 3, 4)), DMA((LAYERS, 2, 2)),
            DMA((LAYERS,)), DMA((LAYERS, GT)), DMA((LAYERS,)), DMA((LAYERS, NP)), DMA((LAYERS, NP, 7)), DMA((LAYERS, NP, 5)),
        ]
        shapes = (hidden_0.shape, hidden_1.shape, flat, flat)
        results = tuple(V(shape, BF16) for shape in shapes)
        out = pl.pallas_call(
            mega_kernel,
            out_shape=results,
            in_specs=[any_spec, any_spec, smem, smem] + [any_spec] * 11,
            out_specs=(vmem,) * 4,
            scratch_shapes=scratch,
            compiler_params=pltpu.CompilerParams(collective_id=0, has_side_effects=True, vmem_limit_bytes=63000000),
        )(hidden_0, hidden_1, positions, lengths, cache_k.reshape(flat), cache_v.reshape(flat), norm_attn, norm_mlp,
          w_query, w_key, w_value, w_out, w_gate, w_up, w_down)
        return out[0], out[1], out[2].reshape(cache_shape), out[3].reshape(cache_shape)

    return jax.shard_map(device_program, mesh=mesh,
                         in_specs=(hidden_spec, hidden_spec, index_spec, index_spec, cache_spec, cache_spec, gain_spec, gain_spec) + (weight_spec,) * 7,
                         out_specs=(hidden_spec, hidden_spec, cache_spec, cache_spec), check_vma=False)
```

```python
import functools

import jax
import jax.numpy as jnp
from jax import lax
from jax.experimental import pallas as pl
from jax.experimental.pallas import tpu as pltpu
from jax.sharding import PartitionSpec as P

ROPE_BASE = 1000000.0
EPS = 1e-05
MESH = pl.DeviceIdType.MESH
F32 = jnp.float32
BF16 = jnp.bfloat16

LAYERS = 2
ROWS = 4
COLS = 2
SEQS = 4
RB = 8
D = 1536
HD = 128
QH = 24
KVH = 4
QW = QH * HD
KVW = KVH * HD
FF = 8192
FK = 4096
WIDTH = 6144
CTX = 128
CW = 1024
KD = 1024
NS = 15

QKV_N = QW + 2 * KVW
KINDS = ['kv'] + ['q'] * 3 + ['o'] * 3 + ['g', 'u'] * 8 + ['d'] * 12
INDEX = [0] + list(range(3)) + list(range(3)) + [i // 2 for i in range(16)] + list(range(12))
PER_LAYER = len(KINDS)
TOTAL = LAYERS * PER_LAYER
BASE = {'qkv': 0, 'o': 4, 'gu': 7, 'd': 23}
NP = 4
DN = 3
GT = 8
GB = 2 * CW
LAG = 1
RELAYED = (1,)


def chunk_of(seq):
    if seq >= TOTAL:
        return None
    layer, pos = divmod(seq, PER_LAYER)
    return layer, KINDS[pos], INDEX[pos]


def mega_kernel(h0, h1, positions, lengths, ck, cv, na, nm, wq, wk, wv, wo, wg, wu, wd,
                out0, out1, kbuf, vbuf,
                wbuf, hbuf, gabuf, gmbuf, nbuf, abuf, xown,
                q_scr, kn_scr, vn_scr, o_scr, lim_scr, cos_scr, sin_scr,
                is_send, is_recv, xi_send, xi_recv,
                qkv_s, qkv_r, o_s, o_r, gd_s, gd_r, gk, gx_s, gx_r, d_s, d_r, dacc,
                ao_s, ao_r, x_s, x_r, aa_s, aa_r, aa_m, st_s, st_r,
                wsem, lsem, isem, xisem, rssem, rrsem, assem, arsem, stsem, gdsem, gdrem, gxsem, gxrem, acsem, acrem):
    c = lax.axis_index('col')
    r = lax.axis_index('row')
    rep = lax.axis_index('rep')
    me = c * ROWS + r
    home = c == r // 2

    def dev(cc, rr):
        return (rep, cc, rr)

    small = [pltpu.make_async_copy(h0, hbuf.at[0], lsem.at[0]),
             pltpu.make_async_copy(h1, hbuf.at[1], lsem.at[1]),
             pltpu.make_async_copy(na, gabuf, lsem.at[2]),
             pltpu.make_async_copy(nm, gmbuf, lsem.at[3]),
             pltpu.make_async_copy(ck, kbuf, lsem.at[4]),
             pltpu.make_async_copy(cv, vbuf, lsem.at[5])]
    for copy in small[:4]:
        copy.start()

    def weight_copy(layer, kind, idx, slot):
        if kind == 'd':
            k, n = idx // DN, idx % DN
            src = wd.at[layer, pl.ds(pl.multiple_of(k * KD, KD), KD), pl.ds(pl.multiple_of(n * CW, CW), CW)]
            return [pltpu.make_async_copy(src, wbuf.at[slot, pl.ds(0, KD)], wsem.at[slot])]
        if kind == 'kv':
            return [pltpu.make_async_copy(ref.at[layer], wbuf.at[slot, :, pl.ds(i * KVW, KVW)], wsem.at[slot])
                    for i, ref in enumerate((wk, wv))]
        ref = {'q': wq, 'o': wo, 'g': wg, 'u': wu}[kind]
        if kind in ('g', 'u'):
            idx = 4 * (idx % 2) + idx // 2
        src = ref.at[layer, :, pl.ds(pl.multiple_of(idx * CW, CW), CW)]
        return [pltpu.make_async_copy(src, wbuf.at[slot], wsem.at[slot])]

    def weight_wait(down, slot):
        if down:
            pltpu.make_async_copy(wd.at[0, pl.ds(0, KD), pl.ds(0, CW)], wbuf.at[slot, pl.ds(0, KD)], wsem.at[slot]).wait()
        else:
            pltpu.make_async_copy(wq.at[0, :, pl.ds(0, CW)], wbuf.at[slot], wsem.at[slot]).wait()

    def issue_initial(lo, hi):
        seq = lo
        while seq < hi:
            layer, kind, idx = chunk_of(seq)
            for copy in weight_copy(layer, kind, idx, seq % NS):
                copy.start(priority=1)
            seq += 1

    issue_initial(0, 4)
    for copy in small[4:]:
        copy.start()
    issue_initial(4, NS)

    def run_phase(layer, base, lo, iters, per, down, body):
        start = layer * PER_LAYER + base

        def future(t):
            return [chunk_of(start + t * per + e + NS) for e in range(per)]

        def signature(t):
            return [None if f is None else f[:2] for f in future(t)]

        t = lo
        while t < iters:
            end = t + 1
            while end < iters and signature(end) == signature(t):
                end += 1
            first = future(t)
            step = [0] * per
            if end - t > 1:
                nxt = future(t + 1)
                step = [0 if f is None else g[2] - f[2] for f, g in zip(first, nxt)]
                for tt in range(t, end):
                    for f, s, g in zip(first, step, future(tt)):
                        assert f is None or f[2] + s * (tt - t) == g[2]

            def one(i, carry, t=t, first=first, step=step):
                slots = [lax.rem(start + i * per + e, NS) for e in range(per)]
                for s in slots:
                    weight_wait(down, s)
                body(i, slots)
                for f, st, s in zip(first, step, slots):
                    if f is not None:
                        for copy in weight_copy(f[0], f[1], f[2] + st * (i - t), s):
                            copy.start(priority=1)
                return carry

            if end - t == 1:
                one(t, 0)
            else:
                lax.fori_loop(t, end, one, 0)
            t = end

    def rs_send(send, recv, ssem, rsem, off, value):
        width = value.shape[1]
        cols = pl.ds(off if isinstance(off, int) else pl.multiple_of(off, width), width)
        for p in range(ROWS):
            send[p, :, cols] = value[p * RB:(p + 1) * RB].astype(BF16)
        for d in (2, 3, 1):
            tgt = lax.rem(r + d, ROWS)
            pltpu.make_async_remote_copy(send.at[tgt, :, cols], recv.at[d - 1, :, cols], ssem, rsem,
                                         device_id=dev(c, tgt), device_id_type=MESH).start()

    def rs_wait_recv(recv, ssem, rsem):
        pltpu.make_async_remote_copy(recv, recv, ssem, rsem, device_id=dev(c, r), device_id_type=MESH).wait_recv()

    def rs_wait_send(send, ssem, rsem):
        ref = send.at[pl.ds(0, 3)]
        pltpu.make_async_remote_copy(ref, ref, ssem, rsem, device_id=dev(c, r), device_id_type=MESH).wait_send()

    def rs_sum(send, recv, lo, hi):
        acc = send[r, :, lo:hi].astype(F32)
        for d in range(ROWS - 1):
            acc = acc + recv[d, :, lo:hi].astype(F32)
        return acc

    def a2a_copy(send, recv, ssem, rsem, j, cc):
        return pltpu.make_async_remote_copy(send.at[j], recv.at[r], ssem.at[j * COLS + cc], rsem.at[r],
                                            device_id=dev(cc, 2 * c + j), device_id_type=MESH)

    def a2a_self(j, cc):
        return jnp.logical_and(c == cc, r == 2 * c + j)

    def a2a_send(send, recv, ssem, rsem, j):
        for cc in range(COLS):
            mine = a2a_self(j, cc)

            @pl.when(jnp.logical_not(mine))
            def _():
                a2a_copy(send, recv, ssem, rsem, j, cc).start()

            @pl.when(mine)
            def _():
                recv[r] = send[j]

    def a2a_wait_recv(send, recv, ssem, rsem):
        for s in range(ROWS):
            @pl.when(jnp.logical_not(jnp.logical_and(home, r == s)))
            def _():
                pltpu.make_async_remote_copy(send.at[0], recv.at[s], ssem.at[0], rsem.at[s],
                                             device_id=dev(c, r), device_id_type=MESH).wait_recv()

    def a2a_wait_send(send, recv, ssem, rsem):
        for j in range(2):
            for cc in range(COLS):
                @pl.when(jnp.logical_not(a2a_self(j, cc)))
                def _():
                    a2a_copy(send, recv, ssem, rsem, j, cc).wait_send()

    core, chip = lax.rem(r, 2), r // 2
    sibling = r + 1 - 2 * core
    across = 2 * (1 - chip) + core

    def act_near(layer, h, j):
        return pltpu.make_async_remote_copy(aa_s.at[layer, h, j], aa_r.at[layer, h, r], acsem.at[layer, h, j], acrem.at[layer, h, r],
                                            device_id=dev(c, 2 * c + j), device_id_type=MESH)

    def act_far(layer, h, j):
        return pltpu.make_async_remote_copy(aa_s.at[layer, h, j], aa_r.at[layer, h, r], acsem.at[layer, h, 2 + j], acrem.at[layer, h, r],
                                            device_id=dev(1 - c, 2 * c + j), device_id_type=MESH)

    def act_hand(layer, h):
        return pltpu.make_async_remote_copy(aa_s.at[layer, h], aa_m.at[layer, h], acsem.at[layer, h, 4], acrem.at[layer, h, 4],
                                            device_id=dev(1 - c, r), device_id_type=MESH)

    def act_forward(layer, h, j):
        return pltpu.make_async_remote_copy(aa_m.at[layer, h, j], aa_r.at[layer, h, r], acsem.at[layer, h, 5 + j], acrem.at[layer, h, r],
                                            device_id=dev(c, 2 * (1 - c) + j), device_id_type=MESH)

    def act_diag(layer, h, j):
        return pltpu.make_async_remote_copy(aa_s.at[layer, h, j], aa_r.at[layer, h, r], acsem.at[layer, h, 2 + j], acrem.at[layer, h, r],
                                            device_id=dev(1 - c, 2 * c + j), device_id_type=MESH)

    def act_send(layer, h):
        @pl.when(jnp.logical_not(home))
        def _():
            if h in RELAYED:
                act_hand(layer, h).start()
            else:
                for j in range(2):
                    act_diag(layer, h, j).start()
            for j in range(2):
                act_near(layer, h, j).start()

        @pl.when(home)
        def _():
            for j in range(2):
                act_far(layer, h, j).start()
            for j in range(2):
                @pl.when(core != j)
                def _():
                    act_near(layer, h, j).start()

                @pl.when(core == j)
                def _():
                    aa_r[layer, h, r] = aa_s[layer, h, j]

    def act_relay(layer, h):
        if h not in RELAYED:
            return

        @pl.when(home)
        def _():
            act_hand(layer, h).wait_recv()
            for j in range(2):
                act_forward(layer, h, j).start()

    def act_wait(layer, h):
        for s in range(ROWS):
            @pl.when(jnp.logical_not(jnp.logical_and(home, r == s)))
            def _():
                pltpu.make_async_remote_copy(aa_s.at[layer, h, 0], aa_r.at[layer, h, s], acsem.at[layer, h, 0], acrem.at[layer, h, s],
                                             device_id=dev(c, r), device_id_type=MESH).wait_recv()

    def act_wait_send(layer, h):
        @pl.when(jnp.logical_not(home))
        def _():
            if h in RELAYED:
                act_hand(layer, h).wait_send()
            else:
                for j in range(2):
                    act_diag(layer, h, j).wait_send()
            for j in range(2):
                act_near(layer, h, j).wait_send()

        @pl.when(home)
        def _():
            for j in range(2):
                act_far(layer, h, j).wait_send()
                if h in RELAYED:
                    act_forward(layer, h, j).wait_send()

                @pl.when(core != j)
                def _():
                    act_near(layer, h, j).wait_send()

    def stat_copy(send, recv, ssem, rsem, e):
        tgt = lax.rem(me + e, COLS * ROWS)
        return pltpu.make_async_remote_copy(send, recv.at[me], ssem, rsem,
                                            device_id=dev(tgt // ROWS, lax.rem(tgt, ROWS)), device_id_type=MESH)

    barrier = pltpu.get_barrier_semaphore()
    for e in range(1, COLS * ROWS):
        tgt = lax.rem(me + e, COLS * ROWS)
        pl.semaphore_signal(barrier, inc=1, device_id=dev(tgt // ROWS, lax.rem(tgt, ROWS)), device_id_type=MESH)
    pl.semaphore_wait(barrier, COLS * ROWS - 1)

    for copy in small[:4]:
        copy.wait()
    h0v = hbuf[0].astype(F32)
    h1v = hbuf[1].astype(F32)
    blocks = [jnp.concatenate([h0v[4 * p:4 * p + 4], h1v[4 * p:4 * p + 4]], axis=0) for p in range(ROWS)]
    lane_block = jnp.right_shift(lax.broadcasted_iota(jnp.int32, (RB, 128), 1), 5)
    packed = jnp.zeros((RB, 128), F32)
    for p in range(ROWS):
        packed = jnp.where(lane_block == p, jnp.sum(blocks[p] * blocks[p], axis=1, keepdims=True), packed)
    is_send[...] = packed
    for d in (2, 3, 1):
        tgt = lax.rem(r + d, ROWS)
        pltpu.make_async_remote_copy(is_send, is_recv.at[d - 1], isem.at[0], isem.at[1],
                                     device_id=dev(c, tgt), device_id_type=MESH).start()
    for p in range(ROWS):
        xi_send[p] = blocks[p].astype(BF16)

    @pl.when(home)
    def _():
        for d in range(1, ROWS):
            tgt = lax.rem(r + d, ROWS)
            pltpu.make_async_remote_copy(xi_send.at[tgt], xi_recv.at[lax.rem(r, 2)], xisem.at[0], xisem.at[1 + lax.rem(r, 2)],
                                         device_id=dev(c, tgt), device_id_type=MESH).start()
        xi_recv[lax.rem(r, 2)] = xi_send[r]

    rowi = lax.broadcasted_iota(jnp.int32, (RB, HD), 0)
    lane = lax.broadcasted_iota(jnp.int32, (RB, HD), 1)
    step_id = (rowi >= SEQS).astype(jnp.int32)
    seq_id = rowi - SEQS * step_id
    pos = step_id
    for b in range(SEQS):
        pos = pos + jnp.where(seq_id == b, positions[b], 0)
    half = (lane >= HD // 2)
    freq_i = jnp.where(half, lane - HD // 2, lane).astype(F32)
    inv_freq = jnp.exp(freq_i * (-13.815510557964274 / 64.0))
    angle = pos.astype(F32) * inv_freq
    cos_scr[...] = jnp.cos(angle)
    sine = jnp.sin(angle)
    sin_scr[...] = jnp.where(half, sine, -sine)

    srow = lax.broadcasted_iota(jnp.int32, (2 * QH, CTX * KVH), 0)
    scol = lax.broadcasted_iota(jnp.int32, (2 * QH, CTX * KVH), 1)
    srow_step = (srow >= QH).astype(jnp.int32)
    srow_h = srow - QH * srow_step
    srow_kv = (srow_h >= 6).astype(jnp.int32) + (srow_h >= 12).astype(jnp.int32) + (srow_h >= 18).astype(jnp.int32)
    slot = jnp.right_shift(scol, 2)
    kv_of = jnp.bitwise_and(scol, 3)
    lim_scr[...] = jnp.where(kv_of == srow_kv, slot - srow_step, 1 << 20)

    pltpu.make_async_remote_copy(is_recv, is_recv, isem.at[0], isem.at[1], device_id=dev(c, r), device_id_type=MESH).wait_recv()

    def normalise(p, xblock, total, gain):
        scale = lax.rsqrt(total * (1.0 / WIDTH) + EPS)[:, :1]
        return xblock * scale * gain

    def put_rows(dst, parts):
        dst[...] = jnp.concatenate(parts, axis=0).astype(BF16)

    gain = gabuf[0:1, :].astype(F32)
    parts = []
    packed = is_send[...] + is_recv[0] + is_recv[1] + is_recv[2]
    for p in range(ROWS):
        parts.append(normalise(p, blocks[p], packed[:, 32 * p:32 * p + 1], gain))
    put_rows(nbuf, parts)

    for copy in small[4:]:
        copy.wait()

    for layer in range(LAYERS):
        qs, qr = qkv_s.at[layer], qkv_r.at[layer]
        qsem = (rssem.at[layer, 0], rrsem.at[layer, 0])

        def lhs_dots(slots):
            lhs = nbuf[...]
            return jnp.concatenate([jnp.dot(lhs, wbuf[s], preferred_element_type=F32) for s in slots], axis=1)

        early = CW

        def qkv_first(i, slots):
            rs_send(qs, qr, qsem[0], rrsem.at[layer, 3], 0, lhs_dots(slots))

        def qkv_rest(i, slots):
            off = i * CW + early
            rs_send(qs, qr, *qsem, off, lhs_dots(slots))

        run_phase(layer, BASE['qkv'], 0, 1, 1, False, qkv_first)
        run_phase(layer, BASE['qkv'] + 1, 0, 3, 1, False, qkv_rest)
        part = qr.at[:, :, pl.ds(0, early)]
        pltpu.make_async_remote_copy(part, part, qsem[0], rrsem.at[layer, 3], device_id=dev(c, r), device_id_type=MESH).wait_recv()

        cosv, sinv = cos_scr[...], sin_scr[...]

        def rope(block):
            value = block.astype(BF16).astype(F32)
            return (value * cosv + pltpu.roll(value, HD // 2, 1) * sinv).astype(BF16).astype(F32)

        for h in range(KVH):
            kn_scr[h * RB:(h + 1) * RB, :] = rope(rs_sum(qs, qr, h * HD, (h + 1) * HD))
            vn_scr[h * RB:(h + 1) * RB, :] = rs_sum(qs, qr, KVW + h * HD, KVW + (h + 1) * HD)
        def query(lo, hi):
            for h in range(lo, hi):
                q_scr[h * RB:(h + 1) * RB, :] = rope(rs_sum(qs, qr, 2 * KVW + h * HD, 2 * KVW + (h + 1) * HD))

        query(0, 0)
        row_slot = jnp.right_shift(lax.broadcasted_iota(jnp.int32, (CTX * KVH, HD), 0), 2)
        for b in range(SEQS):
            length = lengths[b]

            def updated(cache, new_scr):
                value = cache[layer, b].astype(F32)
                for s in range(2):
                    new = new_scr[pl.ds(b + SEQS * s, KVH, stride=RB), :]
                    tile = jnp.concatenate([new, new], axis=0)
                    full = jnp.broadcast_to(tile[None], (CTX * KVH // 8, 8, HD)).reshape(CTX * KVH, HD)
                    value = jnp.where(row_slot == length + s, full, value)
                return value.astype(BF16)

            kbuf[layer, b] = updated(kbuf, kn_scr)
            vbuf[layer, b] = updated(vbuf, vn_scr)

        part = qr.at[:, :, pl.ds(early, QKV_N - early)]
        pltpu.make_async_remote_copy(part, part, *qsem, device_id=dev(c, r), device_id_type=MESH).wait_recv()
        query(0, QH)
        scores = []
        for b in range(SEQS):
            qb = jnp.concatenate([q_scr[pl.ds(b + SEQS * s, QH, stride=RB), :] for s in range(2)], axis=0).astype(BF16)
            scores.append(lax.dot_general(qb, kbuf[layer, b], (((1,), (1,)), ((), ())), preferred_element_type=F32))
        probs = []
        for b in range(SEQS):
            sc = jnp.where(lim_scr[...] <= lengths[b], scores[b] * (HD ** -0.5), -jnp.inf)
            e = jnp.exp(sc - jnp.max(sc, axis=1, keepdims=True))
            probs.append((e / jnp.sum(e, axis=1, keepdims=True)).astype(BF16))
        outs = [jnp.dot(probs[b], vbuf[layer, b], preferred_element_type=F32) for b in range(SEQS)]
        for b in range(SEQS):
            for s in range(2):
                o_scr[pl.ds(b + SEQS * s, QH, stride=RB), :] = outs[b][s * QH:(s + 1) * QH]
        aos, aor = ao_s.at[layer], ao_r.at[layer]
        aosem = (assem.at[layer, 0], arsem.at[layer, 0])
        for j in range(2):
            for h in range(QH // 2):
                hh = j * (QH // 2) + h
                aos[j, :, h * HD:(h + 1) * HD] = o_scr[hh * RB:(hh + 1) * RB, :].astype(BF16)
            a2a_send(aos, aor, *aosem, j)
        a2a_wait_recv(aos, aor, *aosem)
        put_rows(nbuf, [aor[p].astype(F32) for p in range(ROWS)])

        if layer == 0:
            for j in range(2):
                @pl.when(jnp.logical_not(jnp.logical_and(home, lax.rem(r, 2) == j)))
                def _():
                    pltpu.make_async_remote_copy(xi_send.at[0], xi_recv.at[j], xisem.at[0], xisem.at[1 + j],
                                                 device_id=dev(c, r), device_id_type=MESH).wait_recv()
                xown[:, j * D:(j + 1) * D] = xi_recv[j].astype(F32)

        os_, or_ = o_s.at[layer], o_r.at[layer]
        osem = (rssem.at[layer, 1], rrsem.at[layer, 1])

        def o_body(i, slots):
            lhs = nbuf[...]
            y = [jnp.dot(lhs, wbuf[s], preferred_element_type=F32) for s in slots]
            rs_send(os_, or_, *osem, i * CW, jnp.concatenate(y, axis=1))

        def residual(send, recv, sems, which):
            rs_wait_recv(recv, *sems)
            xs, xr = x_s.at[layer, which], x_r.at[layer, which]
            xsem = (assem.at[layer, 1 + which], arsem.at[layer, 1 + which])
            squares = jnp.zeros((RB, 128), F32)
            for j in range(2):
                update = rs_sum(send, recv, j * D, (j + 1) * D).astype(BF16).astype(F32)
                x = (xown[:, j * D:(j + 1) * D] + update).astype(BF16)
                xs[j] = x
                x = x.astype(F32)
                xown[:, j * D:(j + 1) * D] = x
                a2a_send(xs, xr, *xsem, j)
                sq = x * x
                for k in range(D // 128):
                    squares = squares + sq[:, k * 128:(k + 1) * 128]
            last = layer == LAYERS - 1 and which == 1
            if not last:
                sts, stv = st_s.at[layer, which], st_r.at[layer, which]
                stat = jnp.broadcast_to(jnp.sum(squares, axis=1, keepdims=True), (RB, 128))
                sts[...] = stat
                stv[me] = stat
                for e in range(1, COLS * ROWS):
                    stat_copy(sts, stv, stsem.at[layer, which, 0], stsem.at[layer, which, 1], e).start()
            a2a_wait_recv(xs, xr, *xsem)
            if last:
                return
            seven = stv.at[pl.ds(0, COLS * ROWS - 1)]
            pltpu.make_async_remote_copy(seven, seven, stsem.at[layer, which, 0], stsem.at[layer, which, 1],
                                         device_id=dev(c, r), device_id_type=MESH).wait_recv()
            g = (gmbuf[layer:layer + 1, :] if which == 0 else gabuf[layer + 1:layer + 2, :]).astype(F32)
            parts = []
            for p in ((r, across, sibling, 2 * (1 - chip) + 1 - core) if which == 0 else range(ROWS)):
                parts.append(normalise(p, xr[p].astype(F32), stv[p] + stv[ROWS + p], g))
            put_rows(nbuf, parts)

        run_phase(layer, BASE['o'], 0, 3, 1, False, o_body)
        residual(os_, or_, osem, 0)

        def gu_cols(i):
            return pl.ds(i * GB if isinstance(i, int) else pl.multiple_of(i * GB, GB), GB)

        def gu_body(i, slots):
            lhs = nbuf[...]
            y = jnp.concatenate([jnp.dot(lhs, wbuf[s], preferred_element_type=F32) for s in slots], axis=1)
            cols = gu_cols(i)
            for p in range(2):
                gk[p, :, cols] = y[p * RB:(p + 1) * RB]
                gd_s[layer, p, :, cols] = y[(2 + p) * RB:(3 + p) * RB].astype(BF16)
            pltpu.make_async_remote_copy(gd_s.at[layer, :, :, cols], gd_r.at[layer, :, :, cols], gdsem.at[layer], gdrem.at[layer, i],
                                         device_id=dev(c, sibling), device_id_type=MESH).start()

            @pl.when(i >= LAG)
            def _():
                pair_sum(i - LAG)

        def pair_sum(i):
            cols = gu_cols(i)
            pltpu.make_async_remote_copy(gd_s.at[layer, :, :, cols], gd_r.at[layer, :, :, cols], gdsem.at[layer], gdrem.at[layer, i],
                                         device_id=dev(c, sibling), device_id_type=MESH).wait_recv()
            s0 = gk[0, :, cols] + gd_r[layer, 0, :, cols].astype(F32)
            s1 = gk[1, :, cols] + gd_r[layer, 1, :, cols].astype(F32)
            gk[0, :, cols] = s0
            gx_s[layer, :, cols] = s1.astype(BF16)
            pltpu.make_async_remote_copy(gx_s.at[layer, :, cols], gx_r.at[layer, :, cols], gxsem.at[layer], gxrem.at[layer, i // (GT // NP)],
                                         device_id=dev(c, across), device_id_type=MESH).start()

        def activate(q):
            width = GT // NP * GB
            ref = gx_r.at[layer, :, pl.ds(q * width, width)]
            pltpu.make_async_remote_copy(ref, ref, gxsem.at[layer], gxrem.at[layer, q], device_id=dev(c, r), device_id_type=MESH).wait_recv()
            for j in range(2):
                lo = q * width + j * GB
                mid, hi = lo + CW, lo + GB
                gate = (gk[0, :, lo:mid] + gx_r[layer, :, lo:mid].astype(F32)).astype(BF16).astype(F32)
                up = (gk[0, :, mid:hi] + gx_r[layer, :, mid:hi].astype(F32)).astype(BF16).astype(F32)
                aa_s[layer, q, j] = (gate * jax.nn.sigmoid(gate) * up).astype(BF16)
            act_send(layer, q)

        ds_, dr_ = d_s.at[layer], d_r.at[layer]
        dsem = (rssem.at[layer, 2], rrsem.at[layer, 2])

        def d_part(q):
            def body(first):
                def run(i, slots):
                    lhs = abuf[:, q * KD:(q + 1) * KD]
                    y = jnp.concatenate([jnp.dot(lhs, wbuf[s, 0:KD], preferred_element_type=F32) for s in slots], axis=1)
                    lo, hi = first * CW, (first + len(slots)) * CW
                    if q > 0:
                        y = y + dacc[:, lo:hi]
                    if q < NP - 1:
                        dacc[:, lo:hi] = y
                        return
                    for part in range(lo, hi, CW):
                        rs_send(ds_, dr_, *dsem, part, y[:, part - lo:part - lo + CW])
                return run

            act_wait(layer, q)
            abuf[:, q * KD:(q + 1) * KD] = jnp.concatenate([aa_r[layer, q, p].astype(F32) for p in range(ROWS)], axis=0).astype(BF16)
            for first, count in (((0, DN),) if q < NP - 1 else ((0, 1), (1, 1), (2, 1))):
                run_phase(layer, BASE['d'] + q * DN + first, 0, 1, count, True, body(first))

        run_phase(layer, BASE['gu'], 0, 6, 2, False, gu_body)
        activate(0)
        run_phase(layer, BASE['gu'], 6, GT, 2, False, gu_body)
        activate(1)
        act_relay(layer, 0)
        for i in range(GT - LAG, GT):
            pair_sum(i)
        activate(2)
        act_relay(layer, 1)
        d_part(0)
        activate(3)
        act_relay(layer, 2)
        d_part(1)
        act_relay(layer, 3)
        d_part(2)
        d_part(3)
        residual(ds_, dr_, dsem, 1)

    final = [x_r[LAYERS - 1, 1, p].astype(F32) for p in range(ROWS)]
    out0[...] = jnp.concatenate([f[0:4] for f in final], axis=0).astype(BF16)
    out1[...] = jnp.concatenate([f[4:8] for f in final], axis=0).astype(BF16)

    pltpu.make_async_remote_copy(is_recv, is_recv, isem.at[0], isem.at[1], device_id=dev(c, r), device_id_type=MESH).wait_send()

    @pl.when(home)
    def _():
        three = xi_send.at[pl.ds(0, 3)]
        pltpu.make_async_remote_copy(three, three, xisem.at[0], xisem.at[1], device_id=dev(c, r), device_id_type=MESH).wait_send()

    for layer in range(LAYERS):
        for ph, (send, recv) in enumerate(((qkv_s, qkv_r), (o_s, o_r), (d_s, d_r))):
            rs_wait_send(send.at[layer], rssem.at[layer, ph], rrsem.at[layer, ph])
        for ph, (send, recv) in enumerate(((ao_s.at[layer], ao_r.at[layer]), (x_s.at[layer, 0], x_r.at[layer, 0]),
                                           (x_s.at[layer, 1], x_r.at[layer, 1]))):
            a2a_wait_send(send, recv, assem.at[layer, ph], arsem.at[layer, ph])
        pltpu.make_async_remote_copy(gd_s.at[layer], gd_s.at[layer], gdsem.at[layer], gdrem.at[layer, 0], device_id=dev(c, r), device_id_type=MESH).wait_send()
        pltpu.make_async_remote_copy(gx_s.at[layer], gx_s.at[layer], gxsem.at[layer], gxrem.at[layer, 0], device_id=dev(c, r), device_id_type=MESH).wait_send()
        for h in range(NP):
            act_wait_send(layer, h)
        for which in range(2):
            if layer == LAYERS - 1 and which == 1:
                continue
            seven = st_r.at[layer, which, pl.ds(0, COLS * ROWS - 1)]
            pltpu.make_async_remote_copy(seven, seven, stsem.at[layer, which, 0], stsem.at[layer, which, 1],
                                         device_id=dev(c, r), device_id_type=MESH).wait_send()


def finish_kernel(*refs):
    copies = [pltpu.make_async_copy(refs[i], refs[4 + i], refs[8].at[i]) for i in range(4)]
    for copy in copies:
        copy.start()
    for copy in copies:
        copy.wait()


def solution(mesh):
    hidden_spec = P('rep', 'row')
    index_spec = P(('rep', 'row'))
    cache_spec = P(None, ('rep', 'row'), None, 'col', None)
    gain_spec = P(None, 'row')
    weight_spec = P(None, 'row', 'col')

    def device_program(hidden_0, hidden_1, positions, lengths, cache_k, cache_v, norm_attn, norm_mlp,
                       w_query, w_key, w_value, w_out, w_gate, w_up, w_down):
        cache_shape = cache_k.shape
        flat = (LAYERS, SEQS, CTX * KVH, HD)
        any_spec = pl.BlockSpec(memory_space=pl.ANY)
        smem = pl.BlockSpec(memory_space=pltpu.SMEM)
        vmem = pl.BlockSpec(memory_space=pltpu.VMEM)
        V = pltpu.VMEM
        DMA = pltpu.SemaphoreType.DMA
        scratch = [
            V((NS, D, CW), BF16), V((2, 16, D), BF16),
            V((LAYERS, D), BF16), V((LAYERS, D), BF16), V((ROWS * RB, D), BF16), V((ROWS * RB, FK), BF16), V((RB, QW), F32),
            V((QH * RB, HD), F32), V((KVH * RB, HD), F32), V((KVH * RB, HD), F32), V((QH * RB, HD), F32),
            V((2 * QH, CTX * KVH), jnp.int32), V((RB, HD), F32), V((RB, HD), F32),
            V((RB, 128), F32), V((3, RB, 128), F32), V((ROWS, RB, D), BF16), V((2, RB, D), BF16),
            V((LAYERS, ROWS, RB, QKV_N), BF16), V((LAYERS, 3, RB, QKV_N), BF16),
            V((LAYERS, ROWS, RB, QW), BF16), V((LAYERS, 3, RB, QW), BF16),
            V((LAYERS, 2, RB, 2 * FF), BF16), V((LAYERS, 2, RB, 2 * FF), BF16), V((2, RB, 2 * FF), F32),
            V((LAYERS, RB, 2 * FF), BF16), V((LAYERS, RB, 2 * FF), BF16),
            V((LAYERS, ROWS, RB, QW), BF16), V((LAYERS, 3, RB, QW), BF16), V((ROWS * RB, QW), F32),
            V((LAYERS, 2, RB, D), BF16), V((LAYERS, ROWS, RB, D), BF16),
            V((LAYERS, 2, 2, RB, D), BF16), V((LAYERS, 2, ROWS, RB, D), BF16),
            V((LAYERS, NP, 2, RB, KD), BF16), V((LAYERS, NP, ROWS, RB, KD), BF16), V((LAYERS, NP, 2, RB, KD), BF16),
            V((LAYERS, 2, RB, 128), F32), V((LAYERS, 2, COLS * ROWS, RB, 128), F32),
            DMA((NS,)), DMA((6,)), DMA((2,)), DMA((3,)),
            DMA((LAYERS, 3)), DMA((LAYERS, 4)), DMA((LAYERS, 3, 4)), DMA((LAYERS, 3, 4)), DMA((LAYERS, 2, 2)),
            DMA((LAYERS,)), DMA((LAYERS, GT)), DMA((LAYERS,)), DMA((LAYERS, NP)), DMA((LAYERS, NP, 7)), DMA((LAYERS, NP, 5)),
        ]
        shapes = (hidden_0.shape, hidden_1.shape, flat, flat)
        results = tuple(V(shape, BF16) for shape in shapes)
        out = pl.pallas_call(
            mega_kernel,
            out_shape=results,
            in_specs=[any_spec, any_spec, smem, smem] + [any_spec] * 11,
            out_specs=(vmem,) * 4,
            scratch_shapes=scratch,
            compiler_params=pltpu.CompilerParams(collective_id=0, has_side_effects=True, vmem_limit_bytes=63000000),
        )(hidden_0, hidden_1, positions, lengths, cache_k.reshape(flat), cache_v.reshape(flat), norm_attn, norm_mlp,
          w_query, w_key, w_value, w_out, w_gate, w_up, w_down)
        out = [pltpu.with_memory_space_constraint(o, pltpu.VMEM) for o in out]
        out = pl.pallas_call(
            finish_kernel,
            out_shape=tuple(jax.ShapeDtypeStruct(shape, BF16) for shape in shapes),
            in_specs=[vmem] * 4, out_specs=(any_spec,) * 4, scratch_shapes=[DMA((4,))],
            compiler_params=pltpu.CompilerParams(vmem_limit_bytes=1 << 20),
        )(*out)
        return out[0], out[1], out[2].reshape(cache_shape), out[3].reshape(cache_shape)

    return jax.shard_map(device_program, mesh=mesh,
                         in_specs=(hidden_spec, hidden_spec, index_spec, index_spec, cache_spec, cache_spec, gain_spec, gain_spec) + (weight_spec,) * 7,
                         out_specs=(hidden_spec, hidden_spec, cache_spec, cache_spec), check_vma=False)
```

```python
import functools

import jax
import jax.numpy as jnp
from jax import lax
from jax.experimental import pallas as pl
from jax.experimental.pallas import tpu as pltpu
from jax.sharding import PartitionSpec as P

ROPE_BASE = 1000000.0
EPS = 1e-05
MESH = pl.DeviceIdType.MESH
F32 = jnp.float32
BF16 = jnp.bfloat16

LAYERS = 2
ROWS = 4
COLS = 2
SEQS = 4
RB = 8
D = 1536
HD = 128
QH = 24
KVH = 4
QW = QH * HD
KVW = KVH * HD
FF = 8192
FK = 4096
WIDTH = 6144
CTX = 128
CW = 1024
KD = 1024
NS = 15

QKV_N = QW + 2 * KVW
KINDS = ['kv'] + ['q'] * 3 + ['o'] * 3 + ['g', 'u'] * 8 + ['d'] * 12
INDEX = [0] + list(range(3)) + list(range(3)) + [i // 2 for i in range(16)] + list(range(12))
PER_LAYER = len(KINDS)
TOTAL = LAYERS * PER_LAYER
BASE = {'qkv': 0, 'o': 4, 'gu': 7, 'd': 23}
NP = 4
DN = 3
GT = 8
GB = 2 * CW
LAG = 1
RELAYED = (1,)


def chunk_of(seq):
    if seq >= TOTAL:
        return None
    layer, pos = divmod(seq, PER_LAYER)
    return layer, KINDS[pos], INDEX[pos]


def mega_kernel(h0, h1, positions, lengths, ck, cv, na, nm, wq, wk, wv, wo, wg, wu, wd,
                out0, out1, kbuf, vbuf,
                wbuf, hbuf, gabuf, gmbuf, nbuf, abuf, xown,
                q_scr, kn_scr, vn_scr, o_scr, lim_scr, cos_scr, sin_scr,
                is_send, is_recv, xi_send, xi_recv,
                qkv_s, qkv_r, o_s, o_r, gd_s, gd_r, gk, gx_s, gx_r, d_s, d_r, dacc,
                ao_s, ao_r, x_s, x_r, aa_s, aa_r, aa_m, st_s, st_r,
                wsem, lsem, isem, xisem, rssem, rrsem, assem, arsem, stsem, gdsem, gdrem, gxsem, gxrem, acsem, acrem):
    c = lax.axis_index('col')
    r = lax.axis_index('row')
    rep = lax.axis_index('rep')
    me = c * ROWS + r
    home = c == r // 2

    def dev(cc, rr):
        return (rep, cc, rr)

    small = [pltpu.make_async_copy(h0, hbuf.at[0], lsem.at[0]),
             pltpu.make_async_copy(h1, hbuf.at[1], lsem.at[1]),
             pltpu.make_async_copy(na, gabuf, lsem.at[2]),
             pltpu.make_async_copy(nm, gmbuf, lsem.at[3]),
             pltpu.make_async_copy(ck, kbuf, lsem.at[4]),
             pltpu.make_async_copy(cv, vbuf, lsem.at[5])]
    for copy in small[:4]:
        copy.start()

    def weight_copy(layer, kind, idx, slot):
        if kind == 'd':
            k, n = idx // DN, idx % DN
            src = wd.at[layer, pl.ds(pl.multiple_of(k * KD, KD), KD), pl.ds(pl.multiple_of(n * CW, CW), CW)]
            return [pltpu.make_async_copy(src, wbuf.at[slot, pl.ds(0, KD)], wsem.at[slot])]
        if kind == 'kv':
            return [pltpu.make_async_copy(ref.at[layer], wbuf.at[slot, :, pl.ds(i * KVW, KVW)], wsem.at[slot])
                    for i, ref in enumerate((wk, wv))]
        ref = {'q': wq, 'o': wo, 'g': wg, 'u': wu}[kind]
        if kind in ('g', 'u'):
            idx = 4 * (idx % 2) + idx // 2
        src = ref.at[layer, :, pl.ds(pl.multiple_of(idx * CW, CW), CW)]
        return [pltpu.make_async_copy(src, wbuf.at[slot], wsem.at[slot])]

    def weight_wait(down, slot):
        if down:
            pltpu.make_async_copy(wd.at[0, pl.ds(0, KD), pl.ds(0, CW)], wbuf.at[slot, pl.ds(0, KD)], wsem.at[slot]).wait()
        else:
            pltpu.make_async_copy(wq.at[0, :, pl.ds(0, CW)], wbuf.at[slot], wsem.at[slot]).wait()

    def issue_initial(lo, hi):
        seq = lo
        while seq < hi:
            layer, kind, idx = chunk_of(seq)
            for copy in weight_copy(layer, kind, idx, seq % NS):
                copy.start(priority=1)
            seq += 1

    issue_initial(0, 4)
    for copy in small[4:]:
        copy.start()
    issue_initial(4, NS)

    def run_phase(layer, base, lo, iters, per, down, body):
        start = layer * PER_LAYER + base

        def future(t):
            return [chunk_of(start + t * per + e + NS) for e in range(per)]

        def signature(t):
            return [None if f is None else f[:2] for f in future(t)]

        t = lo
        while t < iters:
            end = t + 1
            while end < iters and signature(end) == signature(t):
                end += 1
            first = future(t)
            step = [0] * per
            if end - t > 1:
                nxt = future(t + 1)
                step = [0 if f is None else g[2] - f[2] for f, g in zip(first, nxt)]
                for tt in range(t, end):
                    for f, s, g in zip(first, step, future(tt)):
                        assert f is None or f[2] + s * (tt - t) == g[2]

            def one(i, carry, t=t, first=first, step=step):
                slots = [lax.rem(start + i * per + e, NS) for e in range(per)]
                for s in slots:
                    weight_wait(down, s)
                body(i, slots)
                for f, st, s in zip(first, step, slots):
                    if f is not None:
                        for copy in weight_copy(f[0], f[1], f[2] + st * (i - t), s):
                            copy.start(priority=1)
                return carry

            if end - t == 1:
                one(t, 0)
            else:
                lax.fori_loop(t, end, one, 0)
            t = end

    def rs_send(send, recv, ssem, rsem, off, value):
        width = value.shape[1]
        cols = pl.ds(off if isinstance(off, int) else pl.multiple_of(off, width), width)
        for p in range(ROWS):
            send[p, :, cols] = value[p * RB:(p + 1) * RB].astype(BF16)
        for d in (2, 3, 1):
            tgt = lax.rem(r + d, ROWS)
            pltpu.make_async_remote_copy(send.at[tgt, :, cols], recv.at[d - 1, :, cols], ssem, rsem,
                                         device_id=dev(c, tgt), device_id_type=MESH).start()

    def rs_wait_recv(recv, ssem, rsem):
        pltpu.make_async_remote_copy(recv, recv, ssem, rsem, device_id=dev(c, r), device_id_type=MESH).wait_recv()

    def rs_wait_send(send, ssem, rsem):
        ref = send.at[pl.ds(0, 3)]
        pltpu.make_async_remote_copy(ref, ref, ssem, rsem, device_id=dev(c, r), device_id_type=MESH).wait_send()

    def rs_sum(send, recv, lo, hi):
        acc = send[r, :, lo:hi].astype(F32)
        for d in range(ROWS - 1):
            acc = acc + recv[d, :, lo:hi].astype(F32)
        return acc

    def a2a_copy(send, recv, ssem, rsem, j, cc):
        return pltpu.make_async_remote_copy(send.at[j], recv.at[r], ssem.at[j * COLS + cc], rsem.at[r],
                                            device_id=dev(cc, 2 * c + j), device_id_type=MESH)

    def a2a_self(j, cc):
        return jnp.logical_and(c == cc, r == 2 * c + j)

    def a2a_send(send, recv, ssem, rsem, j):
        for cc in range(COLS):
            mine = a2a_self(j, cc)

            @pl.when(jnp.logical_not(mine))
            def _():
                a2a_copy(send, recv, ssem, rsem, j, cc).start()

            @pl.when(mine)
            def _():
                recv[r] = send[j]

    def a2a_wait_recv(send, recv, ssem, rsem):
        for s in range(ROWS):
            @pl.when(jnp.logical_not(jnp.logical_and(home, r == s)))
            def _():
                pltpu.make_async_remote_copy(send.at[0], recv.at[s], ssem.at[0], rsem.at[s],
                                             device_id=dev(c, r), device_id_type=MESH).wait_recv()

    def a2a_wait_send(send, recv, ssem, rsem):
        for j in range(2):
            for cc in range(COLS):
                @pl.when(jnp.logical_not(a2a_self(j, cc)))
                def _():
                    a2a_copy(send, recv, ssem, rsem, j, cc).wait_send()

    core, chip = lax.rem(r, 2), r // 2
    sibling = r + 1 - 2 * core
    across = 2 * (1 - chip) + core

    def act_near(layer, h, j):
        return pltpu.make_async_remote_copy(aa_s.at[layer, h, j], aa_r.at[layer, h, r], acsem.at[layer, h, j], acrem.at[layer, h, r],
                                            device_id=dev(c, 2 * c + j), device_id_type=MESH)

    def act_far(layer, h, j):
        return pltpu.make_async_remote_copy(aa_s.at[layer, h, j], aa_r.at[layer, h, r], acsem.at[layer, h, 2 + j], acrem.at[layer, h, r],
                                            device_id=dev(1 - c, 2 * c + j), device_id_type=MESH)

    def act_hand(layer, h):
        return pltpu.make_async_remote_copy(aa_s.at[layer, h], aa_m.at[layer, h], acsem.at[layer, h, 4], acrem.at[layer, h, 4],
                                            device_id=dev(1 - c, r), device_id_type=MESH)

    def act_forward(layer, h, j):
        return pltpu.make_async_remote_copy(aa_m.at[layer, h, j], aa_r.at[layer, h, r], acsem.at[layer, h, 5 + j], acrem.at[layer, h, r],
                                            device_id=dev(c, 2 * (1 - c) + j), device_id_type=MESH)

    def act_diag(layer, h, j):
        return pltpu.make_async_remote_copy(aa_s.at[layer, h, j], aa_r.at[layer, h, r], acsem.at[layer, h, 2 + j], acrem.at[layer, h, r],
                                            device_id=dev(1 - c, 2 * c + j), device_id_type=MESH)

    def act_send(layer, h):
        @pl.when(jnp.logical_not(home))
        def _():
            if h in RELAYED:
                act_hand(layer, h).start()
            else:
                for j in range(2):
                    act_diag(layer, h, j).start()
            for j in range(2):
                act_near(layer, h, j).start()

        @pl.when(home)
        def _():
            for j in range(2):
                act_far(layer, h, j).start()
            for j in range(2):
                @pl.when(core != j)
                def _():
                    act_near(layer, h, j).start()

                @pl.when(core == j)
                def _():
                    aa_r[layer, h, r] = aa_s[layer, h, j]

    def act_relay(layer, h):
        if h not in RELAYED:
            return

        @pl.when(home)
        def _():
            act_hand(layer, h).wait_recv()
            for j in range(2):
                act_forward(layer, h, j).start()

    def act_wait(layer, h):
        for s in range(ROWS):
            @pl.when(jnp.logical_not(jnp.logical_and(home, r == s)))
            def _():
                pltpu.make_async_remote_copy(aa_s.at[layer, h, 0], aa_r.at[layer, h, s], acsem.at[layer, h, 0], acrem.at[layer, h, s],
                                             device_id=dev(c, r), device_id_type=MESH).wait_recv()

    def act_wait_send(layer, h):
        @pl.when(jnp.logical_not(home))
        def _():
            if h in RELAYED:
                act_hand(layer, h).wait_send()
            else:
                for j in range(2):
                    act_diag(layer, h, j).wait_send()
            for j in range(2):
                act_near(layer, h, j).wait_send()

        @pl.when(home)
        def _():
            for j in range(2):
                act_far(layer, h, j).wait_send()
                if h in RELAYED:
                    act_forward(layer, h, j).wait_send()

                @pl.when(core != j)
                def _():
                    act_near(layer, h, j).wait_send()

    def stat_copy(send, recv, ssem, rsem, e):
        tgt = lax.rem(me + e, COLS * ROWS)
        return pltpu.make_async_remote_copy(send, recv.at[me], ssem, rsem,
                                            device_id=dev(tgt // ROWS, lax.rem(tgt, ROWS)), device_id_type=MESH)

    barrier = pltpu.get_barrier_semaphore()
    for e in range(1, COLS * ROWS):
        tgt = lax.rem(me + e, COLS * ROWS)
        pl.semaphore_signal(barrier, inc=1, device_id=dev(tgt // ROWS, lax.rem(tgt, ROWS)), device_id_type=MESH)
    pl.semaphore_wait(barrier, COLS * ROWS - 1)

    for copy in small[:4]:
        copy.wait()
    h0v = hbuf[0].astype(F32)
    h1v = hbuf[1].astype(F32)
    blocks = [jnp.concatenate([h0v[4 * p:4 * p + 4], h1v[4 * p:4 * p + 4]], axis=0) for p in range(ROWS)]
    lane_block = jnp.right_shift(lax.broadcasted_iota(jnp.int32, (RB, 128), 1), 5)
    packed = jnp.zeros((RB, 128), F32)
    for p in range(ROWS):
        packed = jnp.where(lane_block == p, jnp.sum(blocks[p] * blocks[p], axis=1, keepdims=True), packed)
    is_send[...] = packed
    for d in (2, 3, 1):
        tgt = lax.rem(r + d, ROWS)
        pltpu.make_async_remote_copy(is_send, is_recv.at[d - 1], isem.at[0], isem.at[1],
                                     device_id=dev(c, tgt), device_id_type=MESH).start()
    for p in range(ROWS):
        xi_send[p] = blocks[p].astype(BF16)

    @pl.when(home)
    def _():
        for d in range(1, ROWS):
            tgt = lax.rem(r + d, ROWS)
            pltpu.make_async_remote_copy(xi_send.at[tgt], xi_recv.at[lax.rem(r, 2)], xisem.at[0], xisem.at[1 + lax.rem(r, 2)],
                                         device_id=dev(c, tgt), device_id_type=MESH).start()
        xi_recv[lax.rem(r, 2)] = xi_send[r]

    rowi = lax.broadcasted_iota(jnp.int32, (RB, HD), 0)
    lane = lax.broadcasted_iota(jnp.int32, (RB, HD), 1)
    step_id = (rowi >= SEQS).astype(jnp.int32)
    seq_id = rowi - SEQS * step_id
    pos = step_id
    for b in range(SEQS):
        pos = pos + jnp.where(seq_id == b, positions[b], 0)
    half = (lane >= HD // 2)
    freq_i = jnp.where(half, lane - HD // 2, lane).astype(F32)
    inv_freq = jnp.exp(freq_i * (-13.815510557964274 / 64.0))
    angle = pos.astype(F32) * inv_freq
    cos_scr[...] = jnp.cos(angle)
    sine = jnp.sin(angle)
    sin_scr[...] = jnp.where(half, sine, -sine)

    srow = lax.broadcasted_iota(jnp.int32, (2 * QH, CTX * KVH), 0)
    scol = lax.broadcasted_iota(jnp.int32, (2 * QH, CTX * KVH), 1)
    srow_step = (srow >= QH).astype(jnp.int32)
    srow_h = srow - QH * srow_step
    srow_kv = (srow_h >= 6).astype(jnp.int32) + (srow_h >= 12).astype(jnp.int32) + (srow_h >= 18).astype(jnp.int32)
    slot = jnp.right_shift(scol, 2)
    kv_of = jnp.bitwise_and(scol, 3)
    lim_scr[...] = jnp.where(kv_of == srow_kv, slot - srow_step, 1 << 20)

    pltpu.make_async_remote_copy(is_recv, is_recv, isem.at[0], isem.at[1], device_id=dev(c, r), device_id_type=MESH).wait_recv()

    own_lanes = jnp.right_shift(lane, 4) == rowi

    def normalise(p, xblock, total, gain):
        scale = lax.rsqrt(total * (1.0 / WIDTH) + EPS)[:, :1]
        return xblock * scale * gain

    def put_rows(dst, parts):
        dst[...] = jnp.concatenate(parts, axis=0).astype(BF16)

    gain = gabuf[0:1, :].astype(F32)
    parts = []
    packed = is_send[...] + is_recv[0] + is_recv[1] + is_recv[2]
    for p in range(ROWS):
        parts.append(normalise(p, blocks[p], packed[:, 32 * p:32 * p + 1], gain))
    put_rows(nbuf, parts)

    for copy in small[4:]:
        copy.wait()

    for layer in range(LAYERS):
        qs, qr = qkv_s.at[layer], qkv_r.at[layer]
        qsem = (rssem.at[layer, 0], rrsem.at[layer, 0])

        def lhs_dots(slots):
            lhs = nbuf[...]
            return jnp.concatenate([jnp.dot(lhs, wbuf[s], preferred_element_type=F32) for s in slots], axis=1)

        early = CW

        def qkv_first(i, slots):
            rs_send(qs, qr, qsem[0], rrsem.at[layer, 3], 0, lhs_dots(slots))

        def qkv_rest(i, slots):
            off = i * CW + early
            rs_send(qs, qr, *qsem, off, lhs_dots(slots))

        run_phase(layer, BASE['qkv'], 0, 1, 1, False, qkv_first)
        run_phase(layer, BASE['qkv'] + 1, 0, 3, 1, False, qkv_rest)
        part = qr.at[:, :, pl.ds(0, early)]
        pltpu.make_async_remote_copy(part, part, qsem[0], rrsem.at[layer, 3], device_id=dev(c, r), device_id_type=MESH).wait_recv()

        cosv, sinv = cos_scr[...], sin_scr[...]

        def rope(block):
            value = block.astype(BF16).astype(F32)
            return (value * cosv + pltpu.roll(value, HD // 2, 1) * sinv).astype(BF16).astype(F32)

        for h in range(KVH):
            kn_scr[h * RB:(h + 1) * RB, :] = rope(rs_sum(qs, qr, h * HD, (h + 1) * HD))
            vn_scr[h * RB:(h + 1) * RB, :] = rs_sum(qs, qr, KVW + h * HD, KVW + (h + 1) * HD)
        def query(lo, hi):
            for h in range(lo, hi):
                q_scr[h * RB:(h + 1) * RB, :] = rope(rs_sum(qs, qr, 2 * KVW + h * HD, 2 * KVW + (h + 1) * HD))

        query(0, 0)
        row_slot = jnp.right_shift(lax.broadcasted_iota(jnp.int32, (CTX * KVH, HD), 0), 2)
        for b in range(SEQS):
            length = lengths[b]

            def updated(cache, new_scr):
                value = cache[layer, b].astype(F32)
                for s in range(2):
                    new = new_scr[pl.ds(b + SEQS * s, KVH, stride=RB), :]
                    tile = jnp.concatenate([new, new], axis=0)
                    full = jnp.broadcast_to(tile[None], (CTX * KVH // 8, 8, HD)).reshape(CTX * KVH, HD)
                    value = jnp.where(row_slot == length + s, full, value)
                return value.astype(BF16)

            kbuf[layer, b] = updated(kbuf, kn_scr)
            vbuf[layer, b] = updated(vbuf, vn_scr)

        part = qr.at[:, :, pl.ds(early, QKV_N - early)]
        pltpu.make_async_remote_copy(part, part, *qsem, device_id=dev(c, r), device_id_type=MESH).wait_recv()
        query(0, QH)
        scores = []
        for b in range(SEQS):
            qb = jnp.concatenate([q_scr[pl.ds(b + SEQS * s, QH, stride=RB), :] for s in range(2)], axis=0).astype(BF16)
            scores.append(lax.dot_general(qb, kbuf[layer, b], (((1,), (1,)), ((), ())), preferred_element_type=F32))
        probs = []
        for b in range(SEQS):
            sc = jnp.where(lim_scr[...] <= lengths[b], scores[b] * (HD ** -0.5), -jnp.inf)
            e = jnp.exp(sc - jnp.max(sc, axis=1, keepdims=True))
            probs.append((e / jnp.sum(e, axis=1, keepdims=True)).astype(BF16))
        outs = [jnp.dot(probs[b], vbuf[layer, b], preferred_element_type=F32) for b in range(SEQS)]
        for b in range(SEQS):
            for s in range(2):
                o_scr[pl.ds(b + SEQS * s, QH, stride=RB), :] = outs[b][s * QH:(s + 1) * QH]
        aos, aor = ao_s.at[layer], ao_r.at[layer]
        aosem = (assem.at[layer, 0], arsem.at[layer, 0])
        for j in range(2):
            for h in range(QH // 2):
                hh = j * (QH // 2) + h
                aos[j, :, h * HD:(h + 1) * HD] = o_scr[hh * RB:(hh + 1) * RB, :].astype(BF16)
            a2a_send(aos, aor, *aosem, j)
        a2a_wait_recv(aos, aor, *aosem)
        put_rows(nbuf, [aor[p].astype(F32) for p in range(ROWS)])

        if layer == 0:
            for j in range(2):
                @pl.when(jnp.logical_not(jnp.logical_and(home, lax.rem(r, 2) == j)))
                def _():
                    pltpu.make_async_remote_copy(xi_send.at[0], xi_recv.at[j], xisem.at[0], xisem.at[1 + j],
                                                 device_id=dev(c, r), device_id_type=MESH).wait_recv()
                xown[:, j * D:(j + 1) * D] = xi_recv[j].astype(F32)

        os_, or_ = o_s.at[layer], o_r.at[layer]
        osem = (rssem.at[layer, 1], rrsem.at[layer, 1])

        def o_body(i, slots):
            lhs = nbuf[...]
            y = [jnp.dot(lhs, wbuf[s], preferred_element_type=F32) for s in slots]
            rs_send(os_, or_, *osem, i * CW, jnp.concatenate(y, axis=1))

        def residual(send, recv, sems, which):
            rs_wait_recv(recv, *sems)
            xs, xr = x_s.at[layer, which], x_r.at[layer, which]
            xsem = (assem.at[layer, 1 + which], arsem.at[layer, 1 + which])
            squares = jnp.zeros((RB, 128), F32)
            for j in range(2):
                update = rs_sum(send, recv, j * D, (j + 1) * D).astype(BF16).astype(F32)
                x = (xown[:, j * D:(j + 1) * D] + update).astype(BF16)
                xs[j] = x
                x = x.astype(F32)
                xown[:, j * D:(j + 1) * D] = x
                a2a_send(xs, xr, *xsem, j)
                sq = x * x
                for k in range(D // 128):
                    squares = squares + sq[:, k * 128:(k + 1) * 128]
            last = layer == LAYERS - 1 and which == 1
            if not last:
                sts, stv = st_s.at[layer, which], st_r.at[layer, which]
                stat = jnp.sum(jnp.where(own_lanes, jnp.sum(squares, axis=1, keepdims=True), 0.0), axis=0, keepdims=True)
                sts[...] = stat
                stv[me] = stat
                for e in range(1, COLS * ROWS):
                    stat_copy(sts, stv, stsem.at[layer, which, 0], stsem.at[layer, which, 1], e).start()
            a2a_wait_recv(xs, xr, *xsem)
            if last:
                return
            seven = stv.at[pl.ds(0, COLS * ROWS - 1)]
            pltpu.make_async_remote_copy(seven, seven, stsem.at[layer, which, 0], stsem.at[layer, which, 1],
                                         device_id=dev(c, r), device_id_type=MESH).wait_recv()
            g = (gmbuf[layer:layer + 1, :] if which == 0 else gabuf[layer + 1:layer + 2, :]).astype(F32)
            parts = []
            for p in ((r, across, sibling, 2 * (1 - chip) + 1 - core) if which == 0 else range(ROWS)):
                parts.append(normalise(p, xr[p].astype(F32), jnp.max(jnp.where(own_lanes, stv[p] + stv[ROWS + p], 0.0), axis=1, keepdims=True), g))
            put_rows(nbuf, parts)

        run_phase(layer, BASE['o'], 0, 3, 1, False, o_body)
        residual(os_, or_, osem, 0)

        def gu_cols(i):
            return pl.ds(i * GB if isinstance(i, int) else pl.multiple_of(i * GB, GB), GB)

        def gu_body(i, slots):
            lhs = nbuf[...]
            y = jnp.concatenate([jnp.dot(lhs, wbuf[s], preferred_element_type=F32) for s in slots], axis=1)
            cols = gu_cols(i)
            for p in range(2):
                gk[p, :, cols] = y[p * RB:(p + 1) * RB]
                gd_s[layer, p, :, cols] = y[(2 + p) * RB:(3 + p) * RB].astype(BF16)
            pltpu.make_async_remote_copy(gd_s.at[layer, :, :, cols], gd_r.at[layer, :, :, cols], gdsem.at[layer], gdrem.at[layer, i],
                                         device_id=dev(c, sibling), device_id_type=MESH).start()

            @pl.when(i >= LAG)
            def _():
                pair_sum(i - LAG)

        def pair_sum(i):
            cols = gu_cols(i)
            pltpu.make_async_remote_copy(gd_s.at[layer, :, :, cols], gd_r.at[layer, :, :, cols], gdsem.at[layer], gdrem.at[layer, i],
                                         device_id=dev(c, sibling), device_id_type=MESH).wait_recv()
            s0 = gk[0, :, cols] + gd_r[layer, 0, :, cols].astype(F32)
            s1 = gk[1, :, cols] + gd_r[layer, 1, :, cols].astype(F32)
            gk[0, :, cols] = s0
            gx_s[layer, :, cols] = s1.astype(BF16)
            pltpu.make_async_remote_copy(gx_s.at[layer, :, cols], gx_r.at[layer, :, cols], gxsem.at[layer], gxrem.at[layer, i // (GT // NP)],
                                         device_id=dev(c, across), device_id_type=MESH).start()

        def activate(q):
            width = GT // NP * GB
            ref = gx_r.at[layer, :, pl.ds(q * width, width)]
            pltpu.make_async_remote_copy(ref, ref, gxsem.at[layer], gxrem.at[layer, q], device_id=dev(c, r), device_id_type=MESH).wait_recv()
            for j in range(2):
                lo = q * width + j * GB
                mid, hi = lo + CW, lo + GB
                gate = (gk[0, :, lo:mid] + gx_r[layer, :, lo:mid].astype(F32)).astype(BF16).astype(F32)
                up = (gk[0, :, mid:hi] + gx_r[layer, :, mid:hi].astype(F32)).astype(BF16).astype(F32)
                aa_s[layer, q, j] = (gate * jax.nn.sigmoid(gate) * up).astype(BF16)
            act_send(layer, q)

        ds_, dr_ = d_s.at[layer], d_r.at[layer]
        dsem = (rssem.at[layer, 2], rrsem.at[layer, 2])

        def d_part(q):
            def body(first):
                def run(i, slots):
                    lhs = abuf[:, q * KD:(q + 1) * KD]
                    y = jnp.concatenate([jnp.dot(lhs, wbuf[s, 0:KD], preferred_element_type=F32) for s in slots], axis=1)
                    lo, hi = first * CW, (first + len(slots)) * CW
                    if q > 0:
                        y = y + dacc[:, lo:hi]
                    if q < NP - 1:
                        dacc[:, lo:hi] = y
                        return
                    for part in range(lo, hi, CW):
                        rs_send(ds_, dr_, *dsem, part, y[:, part - lo:part - lo + CW])
                return run

            act_wait(layer, q)
            abuf[:, q * KD:(q + 1) * KD] = jnp.concatenate([aa_r[layer, q, p].astype(F32) for p in range(ROWS)], axis=0).astype(BF16)
            for first, count in (((0, DN),) if q < NP - 1 else ((0, 1), (1, 1), (2, 1))):
                run_phase(layer, BASE['d'] + q * DN + first, 0, 1, count, True, body(first))

        run_phase(layer, BASE['gu'], 0, 6, 2, False, gu_body)
        activate(0)
        run_phase(layer, BASE['gu'], 6, GT, 2, False, gu_body)
        activate(1)
        act_relay(layer, 0)
        for i in range(GT - LAG, GT):
            pair_sum(i)
        activate(2)
        act_relay(layer, 1)
        d_part(0)
        activate(3)
        act_relay(layer, 2)
        d_part(1)
        act_relay(layer, 3)
        d_part(2)
        d_part(3)
        residual(ds_, dr_, dsem, 1)

    final = [x_r[LAYERS - 1, 1, p].astype(F32) for p in range(ROWS)]
    out0[...] = jnp.concatenate([f[0:4] for f in final], axis=0).astype(BF16)
    out1[...] = jnp.concatenate([f[4:8] for f in final], axis=0).astype(BF16)

    pltpu.make_async_remote_copy(is_recv, is_recv, isem.at[0], isem.at[1], device_id=dev(c, r), device_id_type=MESH).wait_send()

    @pl.when(home)
    def _():
        three = xi_send.at[pl.ds(0, 3)]
        pltpu.make_async_remote_copy(three, three, xisem.at[0], xisem.at[1], device_id=dev(c, r), device_id_type=MESH).wait_send()

    for layer in range(LAYERS):
        for ph, (send, recv) in enumerate(((qkv_s, qkv_r), (o_s, o_r), (d_s, d_r))):
            rs_wait_send(send.at[layer], rssem.at[layer, ph], rrsem.at[layer, ph])
        for ph, (send, recv) in enumerate(((ao_s.at[layer], ao_r.at[layer]), (x_s.at[layer, 0], x_r.at[layer, 0]),
                                           (x_s.at[layer, 1], x_r.at[layer, 1]))):
            a2a_wait_send(send, recv, assem.at[layer, ph], arsem.at[layer, ph])
        pltpu.make_async_remote_copy(gd_s.at[layer], gd_s.at[layer], gdsem.at[layer], gdrem.at[layer, 0], device_id=dev(c, r), device_id_type=MESH).wait_send()
        pltpu.make_async_remote_copy(gx_s.at[layer], gx_s.at[layer], gxsem.at[layer], gxrem.at[layer, 0], device_id=dev(c, r), device_id_type=MESH).wait_send()
        for h in range(NP):
            act_wait_send(layer, h)
        for which in range(2):
            if layer == LAYERS - 1 and which == 1:
                continue
            seven = st_r.at[layer, which, pl.ds(0, COLS * ROWS - 1)]
            pltpu.make_async_remote_copy(seven, seven, stsem.at[layer, which, 0], stsem.at[layer, which, 1],
                                         device_id=dev(c, r), device_id_type=MESH).wait_send()


def finish_kernel(*refs):
    copies = [pltpu.make_async_copy(refs[i], refs[4 + i], refs[8].at[i]) for i in range(4)]
    for copy in copies:
        copy.start()
    for copy in copies:
        copy.wait()


def solution(mesh):
    hidden_spec = P('rep', 'row')
    index_spec = P(('rep', 'row'))
    cache_spec = P(None, ('rep', 'row'), None, 'col', None)
    gain_spec = P(None, 'row')
    weight_spec = P(None, 'row', 'col')

    def device_program(hidden_0, hidden_1, positions, lengths, cache_k, cache_v, norm_attn, norm_mlp,
                       w_query, w_key, w_value, w_out, w_gate, w_up, w_down):
        cache_shape = cache_k.shape
        flat = (LAYERS, SEQS, CTX * KVH, HD)
        any_spec = pl.BlockSpec(memory_space=pl.ANY)
        smem = pl.BlockSpec(memory_space=pltpu.SMEM)
        vmem = pl.BlockSpec(memory_space=pltpu.VMEM)
        V = pltpu.VMEM
        DMA = pltpu.SemaphoreType.DMA
        scratch = [
            V((NS, D, CW), BF16), V((2, 16, D), BF16),
            V((LAYERS, D), BF16), V((LAYERS, D), BF16), V((ROWS * RB, D), BF16), V((ROWS * RB, FK), BF16), V((RB, QW), F32),
            V((QH * RB, HD), F32), V((KVH * RB, HD), F32), V((KVH * RB, HD), F32), V((QH * RB, HD), F32),
            V((2 * QH, CTX * KVH), jnp.int32), V((RB, HD), F32), V((RB, HD), F32),
            V((RB, 128), F32), V((3, RB, 128), F32), V((ROWS, RB, D), BF16), V((2, RB, D), BF16),
            V((LAYERS, ROWS, RB, QKV_N), BF16), V((LAYERS, 3, RB, QKV_N), BF16),
            V((LAYERS, ROWS, RB, QW), BF16), V((LAYERS, 3, RB, QW), BF16),
            V((LAYERS, 2, RB, 2 * FF), BF16), V((LAYERS, 2, RB, 2 * FF), BF16), V((2, RB, 2 * FF), F32),
            V((LAYERS, RB, 2 * FF), BF16), V((LAYERS, RB, 2 * FF), BF16),
            V((LAYERS, ROWS, RB, QW), BF16), V((LAYERS, 3, RB, QW), BF16), V((ROWS * RB, QW), F32),
            V((LAYERS, 2, RB, D), BF16), V((LAYERS, ROWS, RB, D), BF16),
            V((LAYERS, 2, 2, RB, D), BF16), V((LAYERS, 2, ROWS, RB, D), BF16),
            V((LAYERS, NP, 2, RB, KD), BF16), V((LAYERS, NP, ROWS, RB, KD), BF16), V((LAYERS, NP, 2, RB, KD), BF16),
            V((LAYERS, 2, 1, 128), F32), V((LAYERS, 2, COLS * ROWS, 1, 128), F32),
            DMA((NS,)), DMA((6,)), DMA((2,)), DMA((3,)),
            DMA((LAYERS, 3)), DMA((LAYERS, 4)), DMA((LAYERS, 3, 4)), DMA((LAYERS, 3, 4)), DMA((LAYERS, 2, 2)),
            DMA((LAYERS,)), DMA((LAYERS, GT)), DMA((LAYERS,)), DMA((LAYERS, NP)), DMA((LAYERS, NP, 7)), DMA((LAYERS, NP, 5)),
        ]
        shapes = (hidden_0.shape, hidden_1.shape, flat, flat)
        results = tuple(V(shape, BF16) for shape in shapes)
        out = pl.pallas_call(
            mega_kernel,
            out_shape=results,
            in_specs=[any_spec, any_spec, smem, smem] + [any_spec] * 11,
            out_specs=(vmem,) * 4,
            scratch_shapes=scratch,
            compiler_params=pltpu.CompilerParams(collective_id=0, has_side_effects=True, vmem_limit_bytes=63000000),
        )(hidden_0, hidden_1, positions, lengths, cache_k.reshape(flat), cache_v.reshape(flat), norm_attn, norm_mlp,
          w_query, w_key, w_value, w_out, w_gate, w_up, w_down)
        out = [pltpu.with_memory_space_constraint(o, pltpu.VMEM) for o in out]
        out = pl.pallas_call(
            finish_kernel,
            out_shape=tuple(jax.ShapeDtypeStruct(shape, BF16) for shape in shapes),
            in_specs=[vmem] * 4, out_specs=(any_spec,) * 4, scratch_shapes=[DMA((4,))],
            compiler_params=pltpu.CompilerParams(vmem_limit_bytes=1 << 20),
        )(*out)
        return out[0], out[1], out[2].reshape(cache_shape), out[3].reshape(cache_shape)

    return jax.shard_map(device_program, mesh=mesh,
                         in_specs=(hidden_spec, hidden_spec, index_spec, index_spec, cache_spec, cache_spec, gain_spec, gain_spec) + (weight_spec,) * 7,
                         out_specs=(hidden_spec, hidden_spec, cache_spec, cache_spec), check_vma=False)
```
